8 devices in a mesh: model: 2 (over z, y), data: 4 (over x, core).
Axes of the slice: x: 2, y: 2, z: 1, core: 2. Of those that a mesh axis runs over, the one named last changes fastest.
Arguments:
- grad_qkv: float32 [4, 4, 768, 2304], P('data', None, None, 'model')
- weight_qkv: float32 [4, 768, 2304], P(None, 'data', 'model')
- moment1_qkv: float32 [4, 768, 2304], P(None, 'data', 'model')
- moment2_qkv: float32 [4, 768, 2304], P(None, 'data', 'model')
- grad_proj: float32 [4, 4, 768, 768], P('data', None, 'model')
- weight_proj: float32 [4, 768, 768], P(None, ('model', 'data'))
- moment1_proj: float32 [4, 768, 768], P(None, ('model', 'data'))
- moment2_proj: float32 [4, 768, 768], P(None, ('model', 'data'))
- grad_fcin: float32 [4, 4, 768, 3072], P('data', None, None, 'model')
- weight_fcin: float32 [4, 768, 3072], P(None, 'data', 'model')
- moment1_fcin: float32 [4, 768, 3072], P(None, 'data', 'model')
- moment2_fcin: float32 [4, 768, 3072], P(None, 'data', 'model')
- grad_fcout: float32 [4, 4, 3072, 768], P('data', None, 'model')
- weight_fcout: float32 [4, 3072, 768], P(None, ('model', 'data'))
- moment1_fcout: float32 [4, 3072, 768], P(None, ('model', 'data'))
- moment2_fcout: float32 [4, 3072, 768], P(None, ('model', 'data'))
Outputs:
- output 1: bfloat16 [4, 768, 2304], P(None, None, 'model')
- output 2: bfloat16 [4, 768, 768], P(None, 'model')
- output 3: bfloat16 [4, 768, 3072], P(None, None, 'model')
- output 4: bfloat16 [4, 3072, 768], P(None, 'model')
- output 5: float32 [4, 768, 2304], P(None, 'data', 'model')
- output 6: float32 [4, 768, 768], P(None, ('model', 'data'))
- output 7: float32 [4, 768, 3072], P(None, 'data', 'model')
- output 8: float32 [4, 3072, 768], P(None, ('model', 'data'))
- output 9: float32 [4, 768, 2304], P(None, 'data', 'model')
- output 10: float32 [4, 768, 768], P(None, ('model', 'data'))
- output 11: float32 [4, 768, 3072], P(None, 'data', 'model')
- output 12: float32 [4, 3072, 768], P(None, ('model', 'data'))
- output 13: float32 [4, 768, 2304], P(None, 'data', 'model')
- output 14: float32 [4, 768, 768], P(None, ('model', 'data'))
- output 15: float32 [4, 768, 3072], P(None, 'data', 'model')
- output 16: float32 [4, 3072, 768], P(None, ('model', 'data'))
All inputs are finite; a program needn't handle non-finite values.
Results may differ from the reference program's by a relative error of at most 0.001.
Values are sent between devices in bfloat16 or wider.
A program may use at most 1 GiB of HBM per device.

```python
import jax
import jax.numpy as jnp

D_MODEL = 768
FF_DIM = 3072
LAYERS = 4
DATA_SIZE = 4
STEP_COUNT = 100

LEARN_RATE = 0.08
BETA_ONE = 0.9
BETA_TWO = 0.999
ADAM_EPS = 1e-6
DECAY_RATE = 0.01
MAX_NORM = 1.0
TILT_RATE = 0.8
KIND_NAMES = ("qkv", "proj", "fcin", "fcout")
KIND_SHAPES = ((D_MODEL, 3 * D_MODEL), (D_MODEL, D_MODEL), (D_MODEL, FF_DIM), (FF_DIM, D_MODEL))


def tilt_profile(num_rows, num_cols):
    row_pos = (jnp.arange(num_rows, dtype=jnp.float32) + 0.5) / num_rows
    col_pos = (jnp.arange(num_cols, dtype=jnp.float32) + 0.5) / num_cols
    row_scale = jnp.exp(TILT_RATE * (2.0 * row_pos - 1.0))
    col_scale = jnp.exp(TILT_RATE * (2.0 * col_pos - 1.0))
    return row_scale[:, None] * col_scale[None, :]


def setup_inputs(seed: int = 0) -> dict:
    base_key = jax.random.key(seed)
    norm_ratio = jax.random.uniform(jax.random.fold_in(base_key, 100), (), jnp.float32, 2.5, 4.5)
    raw_grads = []
    grad_scales = []
    total_sq = jnp.zeros((), jnp.float32)
    for kind_idx, shape_pair in enumerate(KIND_SHAPES):
        num_rows, num_cols = shape_pair
        kind_keys = jax.random.split(jax.random.fold_in(base_key, kind_idx), 7)
        grad_scale = jnp.exp(jax.random.uniform(kind_keys[0], (LAYERS, 1, 1), jnp.float32, -1.1, 1.1))
        common = jax.random.normal(kind_keys[1], (1, LAYERS, num_rows, num_cols), jnp.float32)
        dev_noise = jax.random.normal(kind_keys[2], (DATA_SIZE, LAYERS, num_rows, num_cols), jnp.float32)
        raw_grad = grad_scale * (common + dev_noise)
        mean_grad = jnp.mean(raw_grad, axis=0)
        total_sq = total_sq + jnp.sum(mean_grad * mean_grad)
        raw_grads.append(raw_grad)
        grad_scales.append(grad_scale)
    factor = norm_ratio * MAX_NORM / jnp.sqrt(total_sq)
    inputs = {}
    for kind_idx, shape_pair in enumerate(KIND_SHAPES):
        num_rows, num_cols = shape_pair
        kind_name = KIND_NAMES[kind_idx]
        kind_keys = jax.random.split(jax.random.fold_in(base_key, kind_idx), 7)
        profile = tilt_profile(num_rows, num_cols)
        weight_scale = jnp.exp(jax.random.uniform(kind_keys[3], (LAYERS, 1, 1), jnp.float32, -1.1, 1.1)) * num_rows ** -0.5
        clip_scale = grad_scales[kind_idx] * factor / norm_ratio
        shape_full = (LAYERS, num_rows, num_cols)
        inputs["grad_" + kind_name] = raw_grads[kind_idx] * factor
        inputs["weight_" + kind_name] = jax.random.normal(kind_keys[4], shape_full, jnp.float32) * weight_scale * profile
        inputs["moment1_" + kind_name] = jax.random.normal(kind_keys[5], shape_full, jnp.float32) * clip_scale
        inputs["moment2_" + kind_name] = (clip_scale * profile) ** 2 * jax.random.uniform(kind_keys[6], shape_full, jnp.float32, 0.5, 1.5)
    return inputs


def lamb_tensor(grad_mean, weight, moment1, moment2, clip_coef):
    clipped = clip_coef * grad_mean
    new_first = BETA_ONE * moment1 + (1.0 - BETA_ONE) * clipped
    new_second = BETA_TWO * moment2 + (1.0 - BETA_TWO) * clipped * clipped
    first_hat = new_first / (1.0 - BETA_ONE ** STEP_COUNT)
    second_hat = new_second / (1.0 - BETA_TWO ** STEP_COUNT)
    update = first_hat / (jnp.sqrt(second_hat) + ADAM_EPS) + DECAY_RATE * weight
    weight_norm = jnp.sqrt(jnp.sum(weight * weight, axis=(1, 2), keepdims=True))
    update_norm = jnp.sqrt(jnp.sum(update * update, axis=(1, 2), keepdims=True))
    new_weight = weight - LEARN_RATE * (weight_norm / update_norm) * update
    return new_weight, new_first, new_second


def reference(grad_qkv, weight_qkv, moment1_qkv, moment2_qkv, grad_proj, weight_proj, moment1_proj, moment2_proj, grad_fcin, weight_fcin, moment1_fcin, moment2_fcin, grad_fcout, weight_fcout, moment1_fcout, moment2_fcout):
    grad_list = (grad_qkv, grad_proj, grad_fcin, grad_fcout)
    states = ((weight_qkv, moment1_qkv, moment2_qkv), (weight_proj, moment1_proj, moment2_proj), (weight_fcin, moment1_fcin, moment2_fcin), (weight_fcout, moment1_fcout, moment2_fcout))
    grad_means = [jnp.sum(grad_stack.astype(jnp.bfloat16).astype(jnp.float32), axis=0) / DATA_SIZE for grad_stack in grad_list]
    total_sq = sum(jnp.sum(grad_mean * grad_mean) for grad_mean in grad_means)
    clip_coef = jnp.minimum(1.0, MAX_NORM / jnp.sqrt(total_sq))
    results = [lamb_tensor(grad_means[kind_idx], states[kind_idx][0], states[kind_idx][1], states[kind_idx][2], clip_coef) for kind_idx in range(4)]
    replicas = [outcome[0].astype(jnp.bfloat16) for outcome in results]
    return (replicas[0], replicas[1], replicas[2], replicas[3], results[0][0], results[1][0], results[2][0], results[3][0], results[0][1], results[1][1], results[2][1], results[3][1], results[0][2], results[1][2], results[2][2], results[3][2])
```

```python
import functools

import jax
import jax.numpy as jnp
from jax import lax
from jax.experimental import pallas as pl
from jax.experimental.pallas import tpu as pltpu
from jax.sharding import PartitionSpec as P

LEARN_RATE = 0.08
BETA_ONE = 0.9
BETA_TWO = 0.999
ADAM_EPS = 1e-6
DECAY_RATE = 0.01
MAX_NORM = 1.0
STEP_COUNT = 100
COLUMN_SPLIT = (True, False, True, False)
MESH = pl.DeviceIdType.MESH
F32, BF16 = jnp.float32, jnp.bfloat16

UNIT_ROWS, UNIT_COLS = 96, 384
CHUNK = 16
KIND_ORDER = (1, 0, 2, 3)
SHARD_ROWS = (96, 192, 192, 384)
SHARD_COLS = (768, 1152, 1536, 768)
LAYERS = 4
COL_BLOCKS = tuple(cols // UNIT_COLS for cols in SHARD_COLS)
BLOCKS = tuple(rows // UNIT_ROWS * (cols // UNIT_COLS) for rows, cols in zip(SHARD_ROWS, SHARD_COLS))
FIRST = tuple(sum(LAYERS * blocks for blocks in BLOCKS[:k]) for k in range(5))
UNITS = FIRST[4]
GROUPS = UNITS // 2
RING = 16
SEND_SLOTS = 8
LAG = 8
RESIDENT = 2 * RING
SENT_GROUPS = FIRST[2] // 2


def grad_spec(col_split):
    return P("data", None, None, "model") if col_split else P("data", None, "model", None)


def state_spec(col_split):
    return P(None, "data", "model") if col_split else P(None, ("model", "data"), None)


def replica_spec(col_split):
    return P(None, None, "model") if col_split else P(None, "model", None)


def adam_direction(grad_mean, weight, moment1, moment2, clip_coef):
    clipped = clip_coef * grad_mean
    new_first = BETA_ONE * moment1 + (1.0 - BETA_ONE) * clipped
    new_second = BETA_TWO * moment2 + (1.0 - BETA_TWO) * clipped * clipped
    first_hat = new_first / (1.0 - BETA_ONE ** STEP_COUNT)
    second_hat = new_second / (1.0 - BETA_TWO ** STEP_COUNT)
    update = first_hat / (jnp.sqrt(second_hat) + ADAM_EPS) + DECAY_RATE * weight
    return update, new_first, new_second


def fold(x):
    parts = [x[8 * i:8 * i + 8, 128 * j:128 * j + 128] for i in range(x.shape[0] // 8) for j in range(x.shape[1] // 128)]
    while len(parts) > 1:
        parts = [a + b for a, b in zip(parts[::2], parts[1::2])] + ([parts[-1]] if len(parts) % 2 else [])
    return parts[0]


def place(kind, index):
    blocks, col_blocks = BLOCKS[kind], COL_BLOCKS[kind]
    layer, block = index // blocks, index % blocks
    row = pl.multiple_of(block // col_blocks * UNIT_ROWS, UNIT_ROWS)
    col = pl.multiple_of(block % col_blocks * UNIT_COLS, UNIT_COLS)
    return layer, row, col


def for_kind(unit, kinds, body):
    for kind in kinds:
        @pl.when((unit >= FIRST[kind]) & (unit < FIRST[kind + 1]))
        def _():
            body(kind, unit - FIRST[kind])


def step_kernel(*refs):
    grads, weights, firsts, seconds = refs[0:4], refs[4:8], refs[8:12], refs[12:16]
    means, reps, shards_in, shards_out, scal = refs[16:20], refs[20:22], refs[22:26], refs[26:30], refs[30]
    (recv, stage, mean, held, ring, note, notes, w_sums, n_sum,
     ring_sem, held_sem, mean_sem, send_sem, recv_sem, rep_send_sem, note_send_sem, note_recv_sem, out_sem) = refs[31:]
    model, data = lax.axis_index("model"), lax.axis_index("data")
    partner = (data, data + 1 - 2 * (data % 2), (data + 2) % 4, 3 - data)

    def unit_at(ref, kind, index, quarter_base=None):
        layer, row, col = place(kind, index)
        if quarter_base is not None:
            row = pl.multiple_of(quarter_base * SHARD_ROWS[kind] + row, UNIT_ROWS)
            return ref.at[layer, pl.ds(row, UNIT_ROWS), pl.ds(col, UNIT_COLS)]
        return ref.at[layer, pl.ds(row, UNIT_ROWS), pl.ds(col, UNIT_COLS)]

    def start_grads(unit):
        def body(kind, index):
            for k in range(4):
                pltpu.make_async_copy(unit_at(grads[kind].at[0], kind, index, partner[k]), ring.at[unit % RING, k], ring_sem.at[unit % RING, k]).start()
        for_kind(unit, range(4), body)

    def start_moments(unit, kinds):
        slot, part = unit // 2 % RING, 2 * (unit % 2)

        def body(kind, index):
            pltpu.make_async_copy(unit_at(firsts[kind], kind, index), ring.at[slot, part], ring_sem.at[slot, part]).start()
            pltpu.make_async_copy(unit_at(seconds[kind], kind, index), ring.at[slot, part + 1], ring_sem.at[slot, part + 1]).start()
        for_kind(unit, kinds, body)

    def start_weight(unit):
        def body(kind, index):
            pltpu.make_async_copy(unit_at(weights[kind], kind, index), held.at[unit], held_sem.at[unit % 32]).start()
        for_kind(unit, range(4), body)

    def start_mean_out(unit):
        def body(kind, index):
            pltpu.make_async_copy(mean.at[unit], unit_at(means[kind], kind, index), mean_sem.at[unit % 16]).start()
        for_kind(unit, range(4), body)

    def wait_ring(slot, part):
        pltpu.make_async_copy(grads[0].at[0, 0, pl.ds(0, UNIT_ROWS), pl.ds(0, UNIT_COLS)], ring.at[slot, part], ring_sem.at[slot, part]).wait()

    def wait_mean_out(unit):
        pltpu.make_async_copy(mean.at[unit], means[0].at[0, pl.ds(0, UNIT_ROWS), pl.ds(0, UNIT_COLS)], mean_sem.at[unit % 16]).wait()

    def stage_slot(group, k):
        return pl.ds((group % SEND_SLOTS * 3 + k - 1) * 2, 2)

    def grad_copy(group, k):
        return pltpu.make_async_remote_copy(
            stage.at[stage_slot(group, k)], recv.at[k - 1, pl.ds(2 * group, 2)], send_sem.at[group % SEND_SLOTS, k - 1],
            recv_sem.at[group, k - 1], device_id=(model, partner[k]), device_id_type=MESH)

    for unit in range(RING):
        start_grads_static(unit, grads, ring, ring_sem, partner)

    barrier = pltpu.get_barrier_semaphore()
    for bits in range(1, 8):
        pl.semaphore_signal(barrier, inc=1, device_id=((model + (bits >> 2)) % 2, partner[bits & 3]), device_id_type=MESH)
    pl.semaphore_wait(barrier, 7)

    n_sum[...] = jnp.zeros_like(n_sum)
    w_sums[...] = jnp.zeros_like(w_sums)

    def convert(group):
        for j in range(2):
            unit = 2 * group + j
            for k in range(4):
                wait_ring(unit % RING, k)

            def rows(i, _):
                at = pl.ds(pl.multiple_of(i * CHUNK, CHUNK), CHUNK)
                mean[unit, at, :] = ring[unit % RING, 0, at, :].astype(BF16).astype(F32)
                for k in (1, 2, 3):
                    stage[(group % SEND_SLOTS * 3 + k - 1) * 2 + j, at, :] = ring[unit % RING, k, at, :].astype(BF16)
                return 0
            lax.fori_loop(0, UNIT_ROWS // CHUNK, rows, 0)

    def add_up(group):
        for k in (1, 2, 3):
            grad_copy(group, k).wait_recv()
        for j in range(2):
            unit = 2 * group + j
            pltpu.make_async_copy(weights[0].at[0, pl.ds(0, UNIT_ROWS), pl.ds(0, UNIT_COLS)], held.at[unit], held_sem.at[unit % 32]).wait()

            @pl.when(unit >= 16)
            def _():
                wait_mean_out(unit - 16)

            def rows(i, sums):
                at = pl.ds(pl.multiple_of(i * CHUNK, CHUNK), CHUNK)
                total = mean[unit, at, :] + recv[0, unit, at, :].astype(F32)
                total = total + (recv[1, unit, at, :].astype(F32) + recv[2, unit, at, :].astype(F32))
                total = total * 0.25
                mean[unit, at, :] = total
                weight = held[unit, at, :]
                return sums[0] + fold(total * total), sums[1] + fold(weight * weight)
            zero = jnp.zeros((8, 128), F32)
            g_part, w_part = lax.fori_loop(0, UNIT_ROWS // CHUNK, rows, (zero, zero))
            n_sum[...] += g_part

            def body(kind, index):
                tensor = LAYERS * kind + index // BLOCKS[kind]
                w_sums[tensor] += w_part
            for_kind(unit, range(4), body)
            start_mean_out(unit)

    def exchange_step(group, _):
        for j in range(2):
            start_weight(2 * group + j)

        @pl.when(group >= SEND_SLOTS)
        def _():
            for k in (1, 2, 3):
                grad_copy(group - SEND_SLOTS, k).wait_send()
        convert(group)

        @pl.when(group >= 1)
        def _():
            for k in (2, 3, 1):
                grad_copy(group - 1, k).start()

        for j in range(2):
            unit = 2 * group + j

            @pl.when(unit + RING < UNITS)
            def _():
                start_grads(unit + RING)

            @pl.when(unit + RING >= UNITS)
            def _():
                for other in range(2):
                    start_moments(2 * (unit + RING - UNITS) + other, (0, 1))

        @pl.when(group >= LAG + 1)
        def _():
            add_up(group - LAG - 1)
        return 0
    lax.fori_loop(0, GROUPS, exchange_step, 0)
    for k in (2, 3, 1):
        grad_copy(GROUPS - 1, k).start()

    def drain_step(group, _):
        add_up(group)
        return 0
    lax.fori_loop(GROUPS - LAG - 1, GROUPS, drain_step, 0)

    def note_copy(index, bits):
        return pltpu.make_async_remote_copy(
            note.at[index], notes.at[index, bits], note_send_sem.at[index, bits], note_recv_sem.at[index, bits],
            device_id=((model + (bits >> 2)) % 2, partner[bits & 3]), device_id_type=MESH)

    def send_note(index):
        for bits in (2, 3, 6, 7, 4, 5, 1):
            note_copy(index, bits).start()

    def read_note(index):
        total = note[index]
        for bits in range(1, 8):
            note_copy(index, bits).wait()
            total = total + notes[index, bits]
        return total

    note[0] = n_sum[...]

    def settle(group, _):
        for k in (1, 2, 3):
            grad_copy(group, k).wait_send()
        return 0
    lax.fori_loop(GROUPS - SEND_SLOTS, GROUPS, settle, 0)
    send_note(0)

    def settle_means(unit, _):
        wait_mean_out(unit)
        return 0
    lax.fori_loop(UNITS - 16, UNITS, settle_means, 0)
    total_sq = jnp.sum(jnp.sum(read_note(0), axis=0, keepdims=True), axis=1, keepdims=True)
    clip = jnp.minimum(1.0, MAX_NORM / jnp.sqrt(total_sq))
    scal[0:8, :] = jnp.broadcast_to(clip, (8, 128))

    def directions(kind, layer_from, layer_to):
        def layer_step(layer, _):
            def block_step(block, total):
                unit = FIRST[kind] + layer * BLOCKS[kind] + block
                slot, part = unit // 2 % RING, 2 * (unit % 2)
                wait_ring(slot, part)
                wait_ring(slot, part + 1)
                for i in range(UNIT_ROWS // CHUNK):
                    at = pl.ds(i * CHUNK, CHUNK)
                    update, _, _ = adam_direction(mean[unit, at, :], held[unit, at, :], ring[slot, part, at, :], ring[slot, part + 1, at, :], clip)
                    mean[unit, at, :] = update
                    total = total + fold(update * update)
                if FIRST[kind] + RESIDENT < UNITS:
                    @pl.when(unit + RESIDENT < UNITS)
                    def _():
                        start_moments(unit + RESIDENT, (2, 3))
                return total
            total = lax.fori_loop(0, BLOCKS[kind], block_step, jnp.zeros((8, 128), F32))
            note[1 + kind, pl.ds(layer, 1), :] = jnp.sum(total, axis=0, keepdims=True)
            note[1 + kind, pl.ds(LAYERS + layer, 1), :] = jnp.sum(w_sums[LAYERS * kind + layer], axis=0, keepdims=True)
            return 0
        lax.fori_loop(layer_from, layer_to, layer_step, 0)

    def ratios(kind):
        norms = jnp.sqrt(jnp.sum(read_note(1 + kind), axis=1, keepdims=True))
        scal[8 + 4 * kind:12 + 4 * kind, :] = jnp.broadcast_to(norms[4:8] / norms[0:4], (4, 128))

    def new_weights(kind, layer_from, layer_to, target):
        def layer_step(layer, _):
            ratio = LEARN_RATE * scal[pl.ds(8 + 4 * kind + layer, 1), :][:, 0:1]

            def block_step(block, _):
                unit = FIRST[kind] + layer * BLOCKS[kind] + block
                for i in range(UNIT_ROWS // CHUNK):
                    at = pl.ds(i * CHUNK, CHUNK)
                    target[unit, at, :] = (held[unit, at, :] - ratio * mean[unit, at, :]).astype(BF16)
                return 0
            lax.fori_loop(0, BLOCKS[kind], block_step, 0)
            return 0
        lax.fori_loop(layer_from, layer_to, layer_step, 0)

    def rep_copy(group, k):
        src = recv.at[1, pl.ds(2 * group, 2)] if k == 3 else stage.at[pl.ds(2 * group, 2)]
        return pltpu.make_async_remote_copy(
            src, recv.at[k - 1, pl.ds(2 * group, 2)], rep_send_sem.at[group, k - 1], recv_sem.at[group, k - 1],
            device_id=(model, partner[1 if k == 3 else k]), device_id_type=MESH)

    def start_replicas(group_from, group_to):
        def body(group, _):
            for k in (2, 1):
                rep_copy(group, k).start()
            return 0
        lax.fori_loop(group_from, group_to, body, 0)

    def forward(group_from, group_to):
        def body(group, _):
            rep_copy(group, 2).wait_recv()
            rep_copy(group, 3).start()
            return 0
        lax.fori_loop(group_from, group_to, body, 0)

    qkv_group, half = FIRST[1] // 2, FIRST[1] // 2 + LAYERS * BLOCKS[1] // 4
    directions(0, 0, 4)
    directions(1, 0, 1)
    send_note(1)
    directions(1, 1, 2)
    ratios(0)
    new_weights(0, 0, 4, stage)
    directions(1, 2, 3)
    start_replicas(0, 2)
    directions(1, 3, 4)
    directions(2, 0, 1)
    send_note(2)
    start_replicas(2, 4)
    directions(2, 1, 3)
    ratios(1)
    new_weights(1, 0, 2, stage)
    directions(2, 3, 4)
    start_replicas(qkv_group, half)
    directions(3, 0, 3)
    new_weights(1, 2, 4, stage)
    directions(3, 3, 4)
    send_note(3)
    send_note(4)
    start_replicas(half, SENT_GROUPS)
    forward(0, half - 2)
    ratios(2)
    ratios(3)
    for kind, outs in ((2, shards_in), (3, shards_out)):
        new_weights(kind, 0, 4, recv.at[0])
    for kind, outs in ((2, shards_in), (3, shards_out)):
        for layer in range(LAYERS):
            for block in range(BLOCKS[kind]):
                row, col = block // COL_BLOCKS[kind] * UNIT_ROWS, block % COL_BLOCKS[kind] * UNIT_COLS
                pltpu.make_async_copy(recv.at[0, FIRST[kind] + layer * BLOCKS[kind] + block], outs[layer].at[0, pl.ds(row, UNIT_ROWS), pl.ds(col, UNIT_COLS)],
                                      held_sem.at[(layer * BLOCKS[kind] + block) % 32]).start()
        for layer in range(LAYERS):
            for block in range(BLOCKS[kind]):
                row, col = block // COL_BLOCKS[kind] * UNIT_ROWS, block % COL_BLOCKS[kind] * UNIT_COLS
                pltpu.make_async_copy(recv.at[0, FIRST[kind] + layer * BLOCKS[kind] + block], outs[layer].at[0, pl.ds(row, UNIT_ROWS), pl.ds(col, UNIT_COLS)],
                                      held_sem.at[(layer * BLOCKS[kind] + block) % 32]).wait()
    forward(half - 2, SENT_GROUPS)

    def replica_out(unit, k, action):
        def body(kind, index):
            src = stage.at[unit] if k == 0 else recv.at[k - 1, unit]
            copy = pltpu.make_async_copy(src, unit_at(reps[kind], kind, index, partner[k]), out_sem.at[unit, k])
            getattr(copy, action)()
        for_kind(unit, (0, 1), body)

    def finish(group, _):
        rep_copy(group, 2).wait_send()
        rep_copy(group, 1).wait()
        rep_copy(group, 3).wait()
        for j in range(2):
            for k in range(4):
                replica_out(2 * group + j, k, "start")
        return 0
    lax.fori_loop(0, SENT_GROUPS, finish, 0)

    def finish_out(unit, _):
        for k in range(4):
            replica_out(unit, k, "wait")
        return 0
    lax.fori_loop(0, 2 * SENT_GROUPS, finish_out, 0)


def start_grads_static(unit, grads, ring, ring_sem, partner):
    kind = next(kind for kind in range(4) if unit < FIRST[kind + 1])
    layer, row, col = (unit - FIRST[kind]) // BLOCKS[kind], (unit - FIRST[kind]) % BLOCKS[kind] // COL_BLOCKS[kind] * UNIT_ROWS, (unit - FIRST[kind]) % BLOCKS[kind] % COL_BLOCKS[kind] * UNIT_COLS
    for k in range(4):
        base = pl.multiple_of(partner[k] * SHARD_ROWS[kind] + row, UNIT_ROWS)
        pltpu.make_async_copy(grads[kind].at[0, layer, pl.ds(base, UNIT_ROWS), pl.ds(col, UNIT_COLS)], ring.at[unit, k], ring_sem.at[unit, k]).start()


def solution(mesh):
    in_specs = []
    for col_split in COLUMN_SPLIT:
        in_specs.extend([grad_spec(col_split), state_spec(col_split), state_spec(col_split), state_spec(col_split)])
    out_specs = tuple([replica_spec(col_split) for col_split in COLUMN_SPLIT] + [state_spec(col_split) for col_split in COLUMN_SPLIT] * 3)
    across = [(i, (i + 2) % 4) for i in range(4)]
    beside = [(i, i + 1 - 2 * (i % 2)) for i in range(4)]

    def device_step(*arrays):
        shape = jax.ShapeDtypeStruct
        shard = [(LAYERS, rows, cols) for rows, cols in zip(SHARD_ROWS, SHARD_COLS)]
        out_shape = (
            [shape(s, F32) for s in shard]
            + [shape((LAYERS, 4 * shard[k][1], shard[k][2]), BF16) for k in (0, 1)]
            + [shape((1,) + shard[k][1:], BF16) for k in (2, 3) for _ in range(LAYERS)]
            + [shape((24, 128), F32)])
        any_spec, vmem_spec = pl.BlockSpec(memory_space=pl.ANY), pl.BlockSpec(memory_space=pltpu.VMEM)
        dma = pltpu.SemaphoreType.DMA
        operands = [arrays[4 * kind + part] for part in range(4) for kind in KIND_ORDER]
        results = pl.pallas_call(
            step_kernel,
            out_shape=out_shape,
            in_specs=[any_spec] * 16,
            out_specs=[any_spec] * (len(out_shape) - 1) + [vmem_spec],
            scratch_shapes=[
                pltpu.VMEM((3, UNITS, UNIT_ROWS, UNIT_COLS), BF16),
                pltpu.VMEM((6 * SEND_SLOTS, UNIT_ROWS, UNIT_COLS), BF16),
                pltpu.VMEM((UNITS, UNIT_ROWS, UNIT_COLS), F32),
                pltpu.VMEM((UNITS, UNIT_ROWS, UNIT_COLS), F32),
                pltpu.VMEM((RING, 4, UNIT_ROWS, UNIT_COLS), F32),
                pltpu.VMEM((5, 8, 128), F32),
                pltpu.VMEM((5, 8, 8, 128), F32),
                pltpu.VMEM((16, 8, 128), F32),
                pltpu.VMEM((8, 128), F32),
                dma((RING, 4)), dma((32,)), dma((16,)), dma((SEND_SLOTS, 3)), dma((GROUPS, 3)), dma((SENT_GROUPS, 3)),
                dma((5, 8)), dma((5, 8)), dma((2 * SENT_GROUPS, 4)),
            ],
            compiler_params=pltpu.CompilerParams(collective_id=0, has_side_effects=True, vmem_limit_bytes=66_900_000),
        )(*operands)
        means, reps, pieces, scal = results[:4], results[4:6], (results[6:10], results[10:14]), results[14]
        clip = scal[0, 0]
        replicas, weights, firsts, seconds = [None] * 4, [None] * 4, [None] * 4, [None] * 4
        me = lax.axis_index("data")
        for slot, kind in enumerate(KIND_ORDER):
            weight = arrays[4 * kind + 1]
            update, firsts[kind], seconds[kind] = adam_direction(means[slot], weight, arrays[4 * kind + 2], arrays[4 * kind + 3], clip)
            ratio = scal[8 + 4 * slot:12 + 4 * slot, 0][:, None, None]
            weights[kind] = weight - LEARN_RATE * ratio * update
        replicas[1], replicas[0] = reps
        for slot, kind in ((2, 2), (3, 3)):
            rows, cols = SHARD_ROWS[slot], SHARD_COLS[slot]
            whole = jnp.zeros((LAYERS, 4 * rows, cols), BF16)
            for layer in range(LAYERS):
                own = pieces[slot - 2][layer]
                far = lax.ppermute(own, "data", across)
                near = lax.ppermute(own, "data", beside)
                far_near = lax.ppermute(far, "data", beside)
                for piece, owner in ((own, me), (near, me + 1 - 2 * (me % 2)), (far, (me + 2) % 4), (far_near, 3 - me)):
                    whole = lax.dynamic_update_slice(whole, piece, (layer, owner * rows, 0))
            replicas[kind] = whole
        return tuple(replicas + weights + firsts + seconds)

    return jax.shard_map(device_step, mesh=mesh, in_specs=tuple(in_specs), out_specs=out_specs, check_vma=False)
```

```python
import functools

import jax
import jax.numpy as jnp
from jax import lax
from jax.experimental import pallas as pl
from jax.experimental.pallas import tpu as pltpu
from jax.sharding import PartitionSpec as P


LEARN_RATE = 0.08
BETA_ONE = 0.9
BETA_TWO = 0.999
ADAM_EPS = 1e-6
DECAY_RATE = 0.01
MAX_NORM = 1.0
STEP_COUNT = 100
COLUMN_SPLIT = (True, False, True, False)
MESH = pl.DeviceIdType.MESH
F32, BF16 = jnp.float32, jnp.bfloat16

UNIT_ROWS, UNIT_COLS = 96, 384
CHUNK = 16
PAIR = 2
TILE = (8, 128)
OWN, NEAR, FAR, CROSS = PARTNERS = range(4)
OTHERS = (NEAR, FAR, CROSS)
PROJ, QKV, FCIN, FCOUT = KINDS = range(4)
KIND_ORDER = (1, 0, 2, 3)
SHARD_ROWS = (96, 192, 192, 384)
SHARD_COLS = (768, 1152, 1536, 768)
LAYERS = 4
COL_BLOCKS = tuple(cols // UNIT_COLS for cols in SHARD_COLS)
BLOCKS = tuple(rows // UNIT_ROWS * (cols // UNIT_COLS) for rows, cols in zip(SHARD_ROWS, SHARD_COLS))
FIRST = tuple(sum(LAYERS * blocks for blocks in BLOCKS[:k]) for k in range(5))
UNITS = FIRST[-1]
GROUPS = UNITS // PAIR
RING = 16
SEND_SLOTS = 8
LAG = 8
RESIDENT = PAIR * RING
SENT_UNITS = FIRST[FCIN]
SENT_GROUPS = SENT_UNITS // PAIR
PIECE_UNITS = FIRST[FCOUT] - FIRST[FCIN]
LATE_GROUPS = 2
RELAYED = SENT_GROUPS - LATE_GROUPS
LAST_ROWS = 192
PIECES = tuple(
    [(layer, 0, SHARD_ROWS[kind]) for layer in range(LAYERS - (kind == FCOUT))]
    + [(LAYERS - 1, 0, SHARD_ROWS[kind] - LAST_ROWS), (LAYERS - 1, SHARD_ROWS[kind] - LAST_ROWS, LAST_ROWS)] * (kind == FCOUT)
    for kind in (FCIN, FCOUT))
PIECE_COUNT = sum(map(len, PIECES))


def grad_spec(col_split):
    return P("data", None, None, "model") if col_split else P("data", None, "model", None)


def state_spec(col_split):
    return P(None, "data", "model") if col_split else P(None, ("model", "data"), None)


def replica_spec(col_split):
    return P(None, None, "model") if col_split else P(None, "model", None)


def adam_direction(grad_mean, weight, moment1, moment2, clip_coef):
    clipped = clip_coef * grad_mean
    new_first = BETA_ONE * moment1 + (1.0 - BETA_ONE) * clipped
    new_second = BETA_TWO * moment2 + (1.0 - BETA_TWO) * clipped * clipped
    first_hat = new_first / (1.0 - BETA_ONE ** STEP_COUNT)
    second_hat = new_second / (1.0 - BETA_TWO ** STEP_COUNT)
    update = first_hat / (jnp.sqrt(second_hat) + ADAM_EPS) + DECAY_RATE * weight
    return update, new_first, new_second


def fold(x):
    sublanes, lanes = TILE
    parts = [x[i:i + sublanes, j:j + lanes] for i in range(0, CHUNK, sublanes) for j in range(0, UNIT_COLS, lanes)]
    return functools.reduce(jnp.add, parts)


def pair(group):
    return pl.ds(PAIR * group, PAIR)


def partners(data):
    return data, data + 1 - PAIR * (data % PAIR), (data + PAIR) % len(PARTNERS), CROSS - data


def zeros():
    return jnp.zeros(TILE, F32)


def split(items, *counts):
    items = iter(items)
    return [[next(items) for _ in range(count)] for count in counts]


def place(kind, index):
    blocks, col_blocks = BLOCKS[kind], COL_BLOCKS[kind]
    layer, block = index // blocks, index % blocks
    row = pl.multiple_of(block // col_blocks * UNIT_ROWS, UNIT_ROWS)
    col = pl.multiple_of(block % col_blocks * UNIT_COLS, UNIT_COLS)
    return layer, row, col


def for_kind(unit, kinds, body):
    for kind in kinds:
        @pl.when((unit >= FIRST[kind]) & (unit < FIRST[kind + 1]))
        def _():
            body(kind, unit - FIRST[kind])


def step_kernel(*refs):
    counts = tuple(map(len, PIECES))
    grads, weights, firsts, seconds, means, reps, in_pieces, out_pieces, rest = split(refs, *[len(KINDS)] * 5, PAIR, *counts, 20)
    pieces = {FCIN: in_pieces, FCOUT: out_pieces}
    (late, scal_out, recv, stage, mean, held, ring, note, notes, w_sums, u_sums, n_sum, scal,
     ring_sem, held_sem, mean_sem, send_sem, recv_sem, rep_send_sem, note_sem) = rest
    model, data = lax.axis_index("model"), lax.axis_index("data")
    partner = partners(data)

    def unit_at(ref, kind, index, quarter_base=None):
        layer, row, col = place(kind, index)
        if quarter_base is not None:
            row = pl.multiple_of(quarter_base * SHARD_ROWS[kind] + row, UNIT_ROWS)
            return ref.at[layer, pl.ds(row, UNIT_ROWS), pl.ds(col, UNIT_COLS)]
        return ref.at[layer, pl.ds(row, UNIT_ROWS), pl.ds(col, UNIT_COLS)]

    def start_grads(unit):
        def body(kind, index):
            for k in PARTNERS:
                pltpu.make_async_copy(unit_at(grads[kind].at[0], kind, index, partner[k]), ring.at[unit % RING, k], ring_sem.at[unit % RING]).start()

        for_kind(unit, KINDS, body)

    def start_moments(unit, kinds):
        slot, part = unit // PAIR % RING, PAIR * (unit % PAIR)

        def body(kind, index):
            pltpu.make_async_copy(unit_at(firsts[kind], kind, index), ring.at[slot, part], ring_sem.at[slot]).start()
            pltpu.make_async_copy(unit_at(seconds[kind], kind, index), ring.at[slot, part + 1], ring_sem.at[slot]).start()

        for_kind(unit, kinds, body)

    def start_weight(unit):
        def body(kind, index):
            pltpu.make_async_copy(unit_at(weights[kind], kind, index), held.at[unit], held_sem.at[unit // PAIR % RING]).start()

        for_kind(unit, KINDS, body)

    def start_mean_out(unit):
        def body(kind, index):
            pltpu.make_async_copy(mean.at[unit], unit_at(means[kind], kind, index), mean_sem.at[unit // PAIR % SEND_SLOTS]).start()

        for_kind(unit, KINDS, body)

    def block(ref, count):
        return ref.at[pl.ds(0, count), pl.ds(0, UNIT_ROWS), pl.ds(0, UNIT_COLS)]

    def wait_ring(slot):
        pltpu.make_async_copy(block(grads[QKV].at[0], len(PARTNERS)), ring.at[slot], ring_sem.at[slot]).wait()

    def wait_weights(group):
        pltpu.make_async_copy(block(weights[QKV], PAIR), held.at[pair(group)], held_sem.at[group % RING]).wait()

    def wait_mean_out(group):
        pltpu.make_async_copy(mean.at[pair(group)], block(means[QKV], PAIR), mean_sem.at[group % SEND_SLOTS]).wait()

    def landed(count):
        return recv.at[0, pl.ds(0, count)]

    def remote(source, target, sent, received, k):
        return pltpu.make_async_remote_copy(source, target, sent, received, device_id=(model, partner[k]), device_id_type=MESH)

    def stage_slot(group, k):
        return group % SEND_SLOTS * len(OTHERS) + k - 1

    def grad_copy(group, k):
        return remote(stage.at[pair(stage_slot(group, k))], recv.at[k - 1, pair(group)], send_sem.at[group % SEND_SLOTS], recv_sem.at[group], k)

    def grad_copies(group):
        count = len(OTHERS) * PAIR
        return remote(landed(count), landed(count), send_sem.at[group % SEND_SLOTS], recv_sem.at[group], FAR)

    early = PAIR * PAIR
    for unit in range(early):
        start_grads_static(unit, grads, ring, ring_sem, partner)

    barrier = pltpu.get_barrier_semaphore()
    peers = [(side, k) for k in (FAR, CROSS, OWN, NEAR) for side in (1, 0) if side or k]

    def device(peer):
        return (model + peer[0]) % PAIR, partner[peer[1]]

    for peer in peers:
        pl.semaphore_signal(barrier, inc=1, device_id=device(peer), device_id_type=MESH)
    pl.semaphore_wait(barrier, len(peers))
    for unit in range(early, RING):
        start_grads_static(unit, grads, ring, ring_sem, partner)

    n_sum[...] = jnp.zeros_like(n_sum)
    note[...] = jnp.zeros_like(note)
    w_sums[...] = jnp.zeros_like(w_sums)
    u_sums[...] = jnp.zeros_like(u_sums)

    def convert(group):
        for j in range(PAIR):
            unit = PAIR * group + j
            wait_ring(unit % RING)

            def rows(i, _):
                at = pl.ds(pl.multiple_of(i * CHUNK, CHUNK), CHUNK)
                for k in OTHERS:
                    stage[PAIR * stage_slot(group, k) + j, at, :] = ring[unit % RING, k, at, :].astype(BF16)
                return 0

            lax.fori_loop(0, UNIT_ROWS // CHUNK, rows, 0)

    def keep_own(group):
        for j in range(PAIR):
            unit = PAIR * group + j

            def rows(i, _):
                at = pl.ds(pl.multiple_of(i * CHUNK, CHUNK), CHUNK)
                mean[unit, at, :] = ring[unit % RING, OWN, at, :].astype(BF16).astype(F32)
                return 0

            lax.fori_loop(0, UNIT_ROWS // CHUNK, rows, 0)

    def add_up(group):
        grad_copies(group).wait_recv()
        wait_weights(group)

        @pl.when(group >= SEND_SLOTS)
        def _():
            wait_mean_out(group - SEND_SLOTS)

        for j in range(PAIR):
            unit = PAIR * group + j

            def rows(i, sums):
                at = pl.ds(pl.multiple_of(i * CHUNK, CHUNK), CHUNK)
                near, far, cross = (recv[k - 1, unit, at, :].astype(F32) for k in OTHERS)
                total = (mean[unit, at, :] + near + (far + cross)) / len(PARTNERS)
                mean[unit, at, :] = total
                weight = held[unit, at, :]
                g_sum, w_sum = sums
                return g_sum + fold(total * total), w_sum + fold(weight * weight)

            g_part, w_part = lax.fori_loop(0, UNIT_ROWS // CHUNK, rows, (zeros(), zeros()))
            n_sum[...] += g_part

            def body(kind, index):
                tensor = LAYERS * kind + index // BLOCKS[kind]
                w_sums[tensor] += w_part

            for_kind(unit, KINDS, body)
            start_mean_out(unit)

    def exchange_step(group, _):
        for j in range(PAIR):
            start_weight(PAIR * group + j)

        @pl.when(group >= SEND_SLOTS)
        def _():
            grad_copies(group - SEND_SLOTS).wait_send()

        convert(group)
        keep_own(group)
        for k in (FAR, CROSS, NEAR):
            grad_copy(group, k).start()

        for j in range(PAIR):
            unit = PAIR * group + j

            @pl.when(unit + RING < UNITS)
            def _():
                start_grads(unit + RING)

            @pl.when(unit + RING >= UNITS)
            def _():
                for other in range(PAIR):
                    start_moments(PAIR * (unit + RING - UNITS) + other, (PROJ, QKV))

        @pl.when(group >= LAG + 1)
        def _():
            add_up(group - LAG - 1)

        return 0

    lax.fori_loop(0, GROUPS, exchange_step, 0)

    def drain_step(group, _):
        add_up(group)
        return 0

    lax.fori_loop(GROUPS - LAG - 1, GROUPS, drain_step, 0)

    n_note, early_note = len(KINDS), len(KINDS) + 1

    def rows_of(index):
        return pl.ds(0, TILE[0] if index in (n_note, early_note) else 1)

    def send_note(index):
        for slot, peer in enumerate(peers):
            pltpu.make_async_remote_copy(
                note.at[index, rows_of(index)], notes.at[index, slot, rows_of(index)], note_sem.at[0, index], note_sem.at[1, index],
                device_id=device(peer), device_id_type=MESH).start()

    def read_note(index):
        arrived = notes.at[index, pl.ds(0, len(peers)), rows_of(index)]
        remote(arrived, arrived, note_sem.at[0, index], note_sem.at[1, index], FAR).wait()
        return note[index] + jnp.sum(notes[index], axis=0)

    note[n_note] = n_sum[...]

    def settle(group, _):
        grad_copies(group).wait_send()
        return 0

    lax.fori_loop(GROUPS - SEND_SLOTS, GROUPS, settle, 0)
    send_note(n_note)

    def settle_means(group, _):
        wait_mean_out(group)
        return 0

    lax.fori_loop(GROUPS - SEND_SLOTS, GROUPS, settle_means, 0)
    total_sq = jnp.sum(jnp.sum(read_note(n_note), axis=0, keepdims=True), axis=1, keepdims=True)
    clip = jnp.minimum(1.0, MAX_NORM / jnp.sqrt(total_sq))
    scal[len(KINDS)] = jnp.broadcast_to(clip, TILE)

    def directions(kind, unit_from, unit_to):
        def group_step(index, _):
            group = FIRST[kind] // PAIR + index
            slot = group % RING
            wait_ring(slot)
            total = zeros()
            for j in range(PAIR):
                unit, part = PAIR * group + j, PAIR * j
                for i in range(0, UNIT_ROWS, CHUNK):
                    at = pl.ds(i, CHUNK)
                    update, _, _ = adam_direction(mean[unit, at, :], held[unit, at, :], ring[slot, part, at, :], ring[slot, part + 1, at, :], clip)
                    mean[unit, at, :] = update
                    total = total + fold(update * update)
            u_sums[LAYERS * kind + PAIR * index // BLOCKS[kind]] += total
            return 0

        lax.fori_loop(unit_from // PAIR, unit_to // PAIR, group_step, 0)

    def refill(unit_from, unit_to):
        def unit_step(unit, _):
            start_moments(unit + RESIDENT, (FCIN, FCOUT))
            return 0

        lax.fori_loop(unit_from, unit_to, unit_step, 0)

    def tensor_sums(kind, layers):
        return [jnp.sum(sums[LAYERS * kind + layer], axis=0, keepdims=True) for sums in (u_sums, w_sums) for layer in range(layers)]

    def write_early_note():
        for row, total in zip((0, LAYERS), tensor_sums(PROJ, 1)):
            note[early_note, row:row + 1, :] = total

    def write_note(kind):
        lane = lax.broadcasted_iota(jnp.int32, (1, TILE[1]), 1)
        packed = jnp.zeros((1, TILE[1]), F32)
        for index, total in enumerate(tensor_sums(kind, LAYERS)):
            packed = jnp.where(lane == index, jnp.sum(total, axis=1, keepdims=True), packed)
        note[kind, :1, :] = packed

    def early_ratio():
        norms = jnp.sqrt(jnp.sum(read_note(early_note), axis=1, keepdims=True))
        scal[PROJ, :1, :] = jnp.broadcast_to(norms[LAYERS:LAYERS + 1] / norms[:1], (1, TILE[1]))

    def ratios(kind):
        norms = jnp.sqrt(read_note(kind)[:1, :])
        for layer in range(LAYERS):
            ratio = norms[:, LAYERS + layer:LAYERS + layer + 1] / norms[:, layer:layer + 1]
            scal[kind, layer:layer + 1, :] = jnp.broadcast_to(ratio, (1, TILE[1]))

    def new_weights(kind, unit_from, unit_to, target):
        def unit_step(index, _):
            unit = FIRST[kind] + index
            ratio = LEARN_RATE * scal[kind, pl.ds(index // BLOCKS[kind], 1), :][:, :1]
            for i in range(0, UNIT_ROWS, CHUNK):
                at = pl.ds(i, CHUNK)
                target[unit, at, :] = (held[unit, at, :] - ratio * mean[unit, at, :]).astype(BF16)
            return 0

        lax.fori_loop(unit_from, unit_to, unit_step, 0)

    near_sem = PAIR * SENT_GROUPS

    def rep_copy(group, k):
        source = recv.at[FAR - 1, pair(group)] if k == CROSS else stage.at[pair(group)]
        arrival = {NEAR: near_sem, FAR: group, CROSS: SENT_GROUPS + group}[k]
        return remote(source, recv.at[k - 1, pair(group)], rep_send_sem.at[k - 1], recv_sem.at[arrival], FAR if k == FAR else NEAR)

    def late_copy(group):
        return remote(stage.at[pair(group)], late.at[pair(group - RELAYED)], rep_send_sem.at[FAR - 1], recv_sem.at[group], FAR)

    def all_copies(k, count):
        return remote(landed(count), landed(count), rep_send_sem.at[k - 1], recv_sem.at[near_sem], NEAR)

    def start_replicas(unit_from, unit_to):
        def body(group, _):
            @pl.when(group < RELAYED)
            def _():
                rep_copy(group, FAR).start()

            @pl.when(group >= RELAYED)
            def _():
                late_copy(group).start()

            rep_copy(group, NEAR).start()
            return 0

        lax.fori_loop(unit_from // PAIR, unit_to // PAIR, body, 0)

    def replicas_out(unit_from, unit_to, k):
        def unit_step(unit, _):
            def body(kind, index):
                source = recv.at[k - 1, unit] if k else stage.at[unit]
                pltpu.make_async_copy(source, unit_at(reps[kind], kind, index, partner[k]), mean_sem.at[k]).start()

            for_kind(unit, (PROJ, QKV), body)
            return 0

        lax.fori_loop(unit_from, unit_to, unit_step, 0)

    def pieces_out(kind):
        for ref, (layer, first, rows) in zip(pieces[kind], PIECES[kind - FCIN]):
            for row in range(0, rows, UNIT_ROWS):
                for column in range(COL_BLOCKS[kind]):
                    unit = FIRST[kind] + layer * BLOCKS[kind] + (first + row) // UNIT_ROWS * COL_BLOCKS[kind] + column
                    target = ref.at[0, pl.ds(row, UNIT_ROWS), pl.ds(column * UNIT_COLS, UNIT_COLS)]
                    pltpu.make_async_copy(recv.at[0, unit], target, mean_sem.at[PAIR + kind]).start()

    proj_end, qkv_end, piece_end = (FIRST[kind + 1] - FIRST[kind] for kind in (PROJ, QKV, FCIN))
    first, half = BLOCKS[PROJ], qkv_end // PAIR
    directions(PROJ, 0, first)
    write_early_note()
    refill(0, first)
    send_note(early_note)
    directions(PROJ, first, proj_end)
    write_note(PROJ)
    directions(QKV, 0, PAIR)
    send_note(PROJ)
    directions(QKV, PAIR, half)
    early_ratio()
    new_weights(PROJ, 0, first, stage)
    refill(first, PAIR * first)
    start_replicas(0, first)
    ratios(PROJ)
    new_weights(PROJ, first, proj_end, stage)
    directions(QKV, half, qkv_end)
    start_replicas(first, PAIR * first)
    write_note(QKV)
    refill(PAIR * first, SENT_UNITS)
    send_note(QKV)
    start_replicas(PAIR * first, proj_end)
    directions(FCIN, 0, piece_end // PAIR)
    ratios(QKV)
    new_weights(QKV, 0, half, stage)
    directions(FCIN, piece_end // PAIR, piece_end // PAIR + PAIR)
    start_replicas(proj_end, proj_end + half)
    directions(FCIN, piece_end // PAIR + PAIR, piece_end)
    refill(FIRST[FCIN], FIRST[FCOUT])
    new_weights(QKV, half, qkv_end, stage)
    directions(FCOUT, 0, piece_end)
    write_note(FCIN)
    write_note(FCOUT)
    replicas_out(0, SENT_UNITS, OWN)
    send_note(FCIN)
    send_note(FCOUT)
    start_replicas(proj_end + half, SENT_UNITS)
    for kind in (FCIN, FCOUT):
        ratios(kind)
        new_weights(kind, 0, piece_end, recv.at[0])
    scal_copy = pltpu.make_async_copy(scal, scal_out, mean_sem.at[len(KINDS) + PAIR])
    scal_copy.start()
    pieces_out(FCIN)
    pieces_out(FCOUT)

    def relay_step(group, _):
        @pl.when(group < RELAYED)
        def _():
            rep_copy(group, FAR).wait_recv()
            rep_copy(group, CROSS).start()
            replicas_out(PAIR * group, PAIR * group + PAIR, FAR)

        @pl.when(group >= 1)
        def _():
            rep_copy(group - 1, CROSS).wait_recv()
            replicas_out(PAIR * group - PAIR, PAIR * group, CROSS)

        return 0

    lax.fori_loop(0, RELAYED + 1, relay_step, 0)
    all_copies(NEAR, SENT_UNITS).wait()
    replicas_out(0, SENT_UNITS, NEAR)
    all_copies(FAR, SENT_UNITS).wait_send()
    all_copies(CROSS, PAIR * RELAYED).wait_send()
    for index, count in enumerate((SENT_UNITS, SENT_UNITS, PAIR * RELAYED, PAIR * RELAYED, PIECE_UNITS, PIECE_UNITS)):
        pltpu.make_async_copy(landed(count), landed(count), mean_sem.at[index]).wait()
    scal_copy.wait()
    for group in range(RELAYED, SENT_GROUPS):
        late_copy(group).wait_recv()


def place_static(kind, index):
    block = index % BLOCKS[kind]
    return index // BLOCKS[kind], block // COL_BLOCKS[kind] * UNIT_ROWS, block % COL_BLOCKS[kind] * UNIT_COLS


def start_grads_static(unit, grads, ring, ring_sem, partner):
    kind = next(kind for kind in KINDS if unit < FIRST[kind + 1])
    layer, row, col = place_static(kind, unit - FIRST[kind])
    for k in PARTNERS:
        base = pl.multiple_of(partner[k] * SHARD_ROWS[kind] + row, UNIT_ROWS)
        pltpu.make_async_copy(grads[kind].at[0, layer, pl.ds(base, UNIT_ROWS), pl.ds(col, UNIT_COLS)], ring.at[unit, k], ring_sem.at[unit]).start()


def assemble_kernel(*refs):
    (proj, qkv, late, late_near), own, near, outs, scratch = split(refs, len(KINDS), PIECE_COUNT, PIECE_COUNT, len(KINDS), 7)
    proj_buf, qkv_buf, in_buf, out_buf, late_sem, whole_sem, piece_sem = scratch
    partner = partners(lax.axis_index("data"))
    copies = []

    def through(source, buffer, target, sem):
        copies.append((pltpu.make_async_copy(source, buffer, sem.at[0]), pltpu.make_async_copy(buffer, target, sem.at[1])))

    for layer in range(LAYERS):
        through(qkv.at[layer], qkv_buf.at[layer], outs[QKV].at[layer], whole_sem.at[layer])
    through(proj, proj_buf, outs[PROJ], whole_sem.at[LAYERS])
    order = [(kind, piece) for kind in (FCIN, FCOUT) for piece in PIECES[kind - FCIN]]
    for number, (kind, (layer, first, rows)) in enumerate(order):
        for k, piece in ((OWN, own[number]), (NEAR, near[number])):
            at = (in_buf if kind == FCIN else out_buf).at[k, pl.ds(layer, 1), pl.ds(first, rows)]
            base = pl.multiple_of(partner[k] * SHARD_ROWS[kind] + first, UNIT_ROWS)
            through(piece, at, outs[kind].at[pl.ds(layer, 1), pl.ds(base, rows)], piece_sem.at[k, number])
    for fetch, _ in copies:
        fetch.start()
    for position, (fetch, store) in enumerate(copies):
        fetch.wait()
        if position == LAYERS - 1:
            fills = []
            for k, source in ((FAR, late), (CROSS, late_near)):
                for unit in range(PAIR * LATE_GROUPS):
                    layer, row, col = place_static(QKV, PAIR * RELAYED + unit - FIRST[QKV])
                    base = pl.multiple_of(partner[k] * SHARD_ROWS[QKV] + row, UNIT_ROWS)
                    target = qkv_buf.at[layer, pl.ds(base, UNIT_ROWS), pl.ds(col, UNIT_COLS)]
                    fills.append(pltpu.make_async_copy(source.at[unit], target, late_sem.at[k - FAR, unit]))
            for fill in fills:
                fill.start()
            for fill in fills:
                fill.wait()
        store.start()
    for _, store in copies:
        store.wait()


def assemble(reps, late, late_near, own, near):
    shape, dma = jax.ShapeDtypeStruct, pltpu.SemaphoreType.DMA
    whole = [(LAYERS, len(PARTNERS) * rows, cols) for rows, cols in zip(SHARD_ROWS, SHARD_COLS)]
    any_spec = pl.BlockSpec(memory_space=pl.ANY)
    operands = [*reps, late, late_near, *own, *near]
    return pl.pallas_call(
        assemble_kernel,
        out_shape=[shape(s, BF16) for s in whole],
        in_specs=[any_spec] * len(operands),
        out_specs=[any_spec] * len(whole),
        scratch_shapes=[
            pltpu.VMEM(whole[PROJ], BF16),
            pltpu.VMEM(whole[QKV], BF16),
            pltpu.VMEM((PAIR, LAYERS, SHARD_ROWS[FCIN], SHARD_COLS[FCIN]), BF16),
            pltpu.VMEM((PAIR, LAYERS, SHARD_ROWS[FCOUT], SHARD_COLS[FCOUT]), BF16),
            dma((PAIR, PAIR * LATE_GROUPS)), dma((LAYERS + 1, PAIR)), dma((PAIR, len(own), PAIR)),
        ],
        compiler_params=pltpu.CompilerParams(vmem_limit_bytes=24_000_000),
        cost_estimate=pl.CostEstimate(flops=12_000_000, bytes_accessed=38_000_000, transcendentals=0),
    )(*operands)


def solution(mesh):
    in_specs = []
    for col_split in COLUMN_SPLIT:
        in_specs.extend([grad_spec(col_split), state_spec(col_split), state_spec(col_split), state_spec(col_split)])
    out_specs = tuple([replica_spec(col_split) for col_split in COLUMN_SPLIT] + [state_spec(col_split) for col_split in COLUMN_SPLIT] * 3)
    across, beside = ([(i, partners(i)[k]) for i in PARTNERS] for k in (FAR, NEAR))

    def device_step(*arrays):
        shape = jax.ShapeDtypeStruct
        shard = [(LAYERS, rows, cols) for rows, cols in zip(SHARD_ROWS, SHARD_COLS)]
        order = [(kind, piece) for kind in (FCIN, FCOUT) for piece in PIECES[kind - FCIN]]
        scal_shape = (len(KINDS) + 1,) + TILE
        out_shape = (
            [shape(s, F32) for s in shard]
            + [shape((LAYERS, len(PARTNERS) * SHARD_ROWS[kind], SHARD_COLS[kind]), BF16) for kind in (PROJ, QKV)]
            + [shape((1, rows, SHARD_COLS[kind]), BF16) for kind, (_, _, rows) in order]
            + [shape((PAIR * LATE_GROUPS, UNIT_ROWS, UNIT_COLS), BF16), shape(scal_shape, F32)])
        any_spec = pl.BlockSpec(memory_space=pl.ANY)
        dma = pltpu.SemaphoreType.DMA
        unit = (UNIT_ROWS, UNIT_COLS)
        messages = len(KINDS) + PAIR
        operands = [arrays[len(KINDS) * kind + part] for part in PARTNERS for kind in KIND_ORDER]
        results = pl.pallas_call(
            step_kernel,
            out_shape=out_shape,
            in_specs=[any_spec] * len(operands),
            out_specs=[any_spec] * len(out_shape),
            scratch_shapes=[
                pltpu.VMEM((len(OTHERS), UNITS) + unit, BF16),
                pltpu.VMEM((len(OTHERS) * PAIR * SEND_SLOTS,) + unit, BF16),
                pltpu.VMEM((UNITS,) + unit, F32),
                pltpu.VMEM((UNITS,) + unit, F32),
                pltpu.VMEM((RING, len(PARTNERS)) + unit, F32),
                pltpu.VMEM((messages,) + TILE, F32),
                pltpu.VMEM((messages, mesh.size - 1) + TILE, F32),
                pltpu.VMEM((LAYERS * len(KINDS),) + TILE, F32),
                pltpu.VMEM((LAYERS * len(KINDS),) + TILE, F32),
                pltpu.VMEM(TILE, F32),
                pltpu.VMEM(scal_shape, F32),
                dma((RING,)), dma((RING,)), dma((SEND_SLOTS,)), dma((SEND_SLOTS,)), dma((GROUPS,)), dma((len(OTHERS),)), dma((PAIR, messages)),
            ],
            compiler_params=pltpu.CompilerParams(collective_id=0, has_side_effects=True, vmem_limit_bytes=66_900_000),
        )(*operands)
        means, reps, pieces, (late, scal) = split(results, len(KINDS), PAIR, PIECE_COUNT, PAIR)
        owners = partners(lax.axis_index("data"))
        state = {}
        clip = scal[len(KINDS), 0, 0]
        for slot, kind in enumerate(KIND_ORDER):
            _, weight, moment1, moment2 = arrays[len(KINDS) * kind:len(KINDS) * kind + len(KINDS)]
            update, new_first, new_second = adam_direction(means[slot], weight, moment1, moment2, clip)
            ratio = jnp.expand_dims(scal[slot, :LAYERS, 0], (1, 2))
            state[kind] = (weight - LEARN_RATE * ratio * update, new_first, new_second)
        far, near = [], []
        for piece in pieces:
            far.append(lax.ppermute(piece, "data", across))
        late_near = lax.ppermute(late, "data", beside)
        near = [lax.ppermute(piece, "data", beside) for piece in pieces]
        replicas = list(assemble(reps, late, late_near, pieces, near))
        for number, (kind, (layer, first, _)) in enumerate(order):
            far_near = lax.ppermute(far[number], "data", beside)
            for piece, k in ((far[number], FAR), (far_near, CROSS)):
                replicas[kind] = lax.dynamic_update_slice(replicas[kind], piece, (layer, owners[k] * SHARD_ROWS[kind] + first, 0))
        outputs = [replicas[KIND_ORDER.index(kind)] for kind in KINDS]
        return tuple(outputs + [state[kind][part] for part in range(len(OTHERS)) for kind in KINDS])

    return jax.shard_map(device_step, mesh=mesh, in_specs=tuple(in_specs), out_specs=out_specs, check_vma=False)
```

```python
import functools

import jax
import jax.numpy as jnp
from jax import lax
from jax.experimental import pallas as pl
from jax.experimental.pallas import tpu as pltpu
from jax.sharding import PartitionSpec as P


LEARN_RATE = 0.08
BETA_ONE = 0.9
BETA_TWO = 0.999
ADAM_EPS = 1e-6
DECAY_RATE = 0.01
MAX_NORM = 1.0
STEP_COUNT = 100
COLUMN_SPLIT = (True, False, True, False)
MESH = pl.DeviceIdType.MESH
F32, BF16 = jnp.float32, jnp.bfloat16

UNIT_ROWS, UNIT_COLS = 96, 384
CHUNK = 16
PAIR = 2
TILE = (8, 128)
OWN, NEAR, FAR, CROSS = PARTNERS = range(4)
OTHERS = (NEAR, FAR, CROSS)
PROJ, QKV, FCIN, FCOUT = KINDS = range(4)
KIND_ORDER = (1, 0, 2, 3)
SHARD_ROWS = (96, 192, 192, 384)
SHARD_COLS = (768, 1152, 1536, 768)
LAYERS = 4
COL_BLOCKS = tuple(cols // UNIT_COLS for cols in SHARD_COLS)
BLOCKS = tuple(rows // UNIT_ROWS * (cols // UNIT_COLS) for rows, cols in zip(SHARD_ROWS, SHARD_COLS))
FIRST = tuple(sum(LAYERS * blocks for blocks in BLOCKS[:k]) for k in range(5))
UNITS = FIRST[-1]
GROUPS = UNITS // PAIR
RING = 16
SEND_SLOTS = 8
LAG = 8
RESIDENT = PAIR * RING
SENT_UNITS = FIRST[FCIN]
SENT_GROUPS = SENT_UNITS // PAIR
PIECE_UNITS = FIRST[FCOUT] - FIRST[FCIN]
LATE_GROUPS = 2
TAIL_GROUPS = 5
TAIL_FIRST = SENT_GROUPS - TAIL_GROUPS
RELAYED = TAIL_FIRST - LATE_GROUPS
LAST_ROWS = 192
PIECES = tuple(
    [(layer, 0, SHARD_ROWS[kind]) for layer in range(LAYERS - (kind == FCOUT))]
    + [(LAYERS - 1, 0, SHARD_ROWS[kind] - LAST_ROWS), (LAYERS - 1, SHARD_ROWS[kind] - LAST_ROWS, LAST_ROWS)] * (kind == FCOUT)
    for kind in (FCIN, FCOUT))
PIECE_COUNT = sum(map(len, PIECES))


def grad_spec(col_split):
    return P("data", None, None, "model") if col_split else P("data", None, "model", None)


def state_spec(col_split):
    return P(None, "data", "model") if col_split else P(None, ("model", "data"), None)


def replica_spec(col_split):
    return P(None, None, "model") if col_split else P(None, "model", None)


def adam_direction(grad_mean, weight, moment1, moment2, clip_coef):
    clipped = clip_coef * grad_mean
    new_first = BETA_ONE * moment1 + (1.0 - BETA_ONE) * clipped
    new_second = BETA_TWO * moment2 + (1.0 - BETA_TWO) * clipped * clipped
    first_hat = new_first / (1.0 - BETA_ONE ** STEP_COUNT)
    second_hat = new_second / (1.0 - BETA_TWO ** STEP_COUNT)
    update = first_hat / (jnp.sqrt(second_hat) + ADAM_EPS) + DECAY_RATE * weight
    return update, new_first, new_second


def fold(x):
    sublanes, lanes = TILE
    parts = [x[i:i + sublanes, j:j + lanes] for i in range(0, CHUNK, sublanes) for j in range(0, UNIT_COLS, lanes)]
    return functools.reduce(jnp.add, parts)


def pair(group):
    return pl.ds(PAIR * group, PAIR)


def partners(data):
    return data, data + 1 - PAIR * (data % PAIR), (data + PAIR) % len(PARTNERS), CROSS - data


def zeros():
    return jnp.zeros(TILE, F32)


def split(items, *counts):
    items = iter(items)
    return [[next(items) for _ in range(count)] for count in counts]


def place(kind, index):
    blocks, col_blocks = BLOCKS[kind], COL_BLOCKS[kind]
    layer, block = index // blocks, index % blocks
    row = pl.multiple_of(block // col_blocks * UNIT_ROWS, UNIT_ROWS)
    col = pl.multiple_of(block % col_blocks * UNIT_COLS, UNIT_COLS)
    return layer, row, col


def for_kind(unit, kinds, body):
    for kind in kinds:
        @pl.when((unit >= FIRST[kind]) & (unit < FIRST[kind + 1]))
        def _():
            body(kind, unit - FIRST[kind])


def step_kernel(*refs):
    counts = tuple(map(len, PIECES))
    grads, weights, firsts, seconds, means, reps, in_pieces, out_pieces, rest = split(refs, *[len(KINDS)] * 5, PAIR, *counts, 22)
    pieces = {FCIN: in_pieces, FCOUT: out_pieces}
    (late, tail, extra, scal_out, recv, stage, mean, held, ring, note, notes, w_sums, u_sums, n_sum, scal,
     ring_sem, held_sem, mean_sem, send_sem, recv_sem, rep_send_sem, note_sem) = rest
    model, data = lax.axis_index("model"), lax.axis_index("data")
    partner = partners(data)
    stays = data % PAIR == 1

    def unit_at(ref, kind, index, quarter_base=None):
        layer, row, col = place(kind, index)
        if quarter_base is not None:
            row = pl.multiple_of(quarter_base * SHARD_ROWS[kind] + row, UNIT_ROWS)
            return ref.at[layer, pl.ds(row, UNIT_ROWS), pl.ds(col, UNIT_COLS)]
        return ref.at[layer, pl.ds(row, UNIT_ROWS), pl.ds(col, UNIT_COLS)]

    def start_grads(unit):
        def body(kind, index):
            for k in PARTNERS:
                pltpu.make_async_copy(unit_at(grads[kind].at[0], kind, index, partner[k]), ring.at[unit % RING, k], ring_sem.at[unit % RING]).start()

        for_kind(unit, KINDS, body)

    def start_moments(unit, kinds):
        slot, part = unit // PAIR % RING, PAIR * (unit % PAIR)

        def body(kind, index):
            pltpu.make_async_copy(unit_at(firsts[kind], kind, index), ring.at[slot, part], ring_sem.at[slot]).start()
            pltpu.make_async_copy(unit_at(seconds[kind], kind, index), ring.at[slot, part + 1], ring_sem.at[slot]).start()

        for_kind(unit, kinds, body)

    def start_weight(unit):
        def body(kind, index):
            pltpu.make_async_copy(unit_at(weights[kind], kind, index), held.at[unit], held_sem.at[unit // PAIR % RING]).start()

        for_kind(unit, KINDS, body)

    def start_mean_out(unit):
        def body(kind, index):
            pltpu.make_async_copy(mean.at[unit], unit_at(means[kind], kind, index), mean_sem.at[unit // PAIR % SEND_SLOTS]).start()

        for_kind(unit, KINDS, body)

    def block(ref, count):
        return ref.at[pl.ds(0, count), pl.ds(0, UNIT_ROWS), pl.ds(0, UNIT_COLS)]

    def wait_ring(slot):
        pltpu.make_async_copy(block(grads[QKV].at[0], len(PARTNERS)), ring.at[slot], ring_sem.at[slot]).wait()

    def wait_weights(group):
        pltpu.make_async_copy(block(weights[QKV], PAIR), held.at[pair(group)], held_sem.at[group % RING]).wait()

    def wait_mean_out(group):
        pltpu.make_async_copy(mean.at[pair(group)], block(means[QKV], PAIR), mean_sem.at[group % SEND_SLOTS]).wait()

    def landed(count):
        return recv.at[0, pl.ds(0, count)]

    def remote(source, target, sent, received, k):
        return pltpu.make_async_remote_copy(source, target, sent, received, device_id=(model, partner[k]), device_id_type=MESH)

    def stage_slot(group, k):
        return group % SEND_SLOTS * len(OTHERS) + k - 1

    def grad_copy(group, k):
        return remote(stage.at[pair(stage_slot(group, k))], recv.at[k - 1, pair(group)], send_sem.at[group % SEND_SLOTS], recv_sem.at[group], k)

    def grad_copies(group):
        count = len(OTHERS) * PAIR
        return remote(landed(count), landed(count), send_sem.at[group % SEND_SLOTS], recv_sem.at[group], FAR)

    early = PAIR * PAIR
    for unit in range(early):
        start_grads_static(unit, grads, ring, ring_sem, partner)

    barrier = pltpu.get_barrier_semaphore()
    peers = [(side, k) for k in (FAR, CROSS, OWN, NEAR) for side in (1, 0) if side or k]

    def device(peer):
        return (model + peer[0]) % PAIR, partner[peer[1]]

    for peer in peers:
        pl.semaphore_signal(barrier, inc=1, device_id=device(peer), device_id_type=MESH)
    pl.semaphore_wait(barrier, len(peers))
    for unit in range(early, RING):
        start_grads_static(unit, grads, ring, ring_sem, partner)

    n_sum[...] = jnp.zeros_like(n_sum)
    note[...] = jnp.zeros_like(note)
    w_sums[...] = jnp.zeros_like(w_sums)
    u_sums[...] = jnp.zeros_like(u_sums)

    def convert(group):
        for j in range(PAIR):
            unit = PAIR * group + j
            wait_ring(unit % RING)

            def rows(i, _):
                at = pl.ds(pl.multiple_of(i * CHUNK, CHUNK), CHUNK)
                for k in OTHERS:
                    stage[PAIR * stage_slot(group, k) + j, at, :] = ring[unit % RING, k, at, :].astype(BF16)
                return 0

            lax.fori_loop(0, UNIT_ROWS // CHUNK, rows, 0)

    def keep_own(group):
        for j in range(PAIR):
            unit = PAIR * group + j

            def rows(i, _):
                at = pl.ds(pl.multiple_of(i * CHUNK, CHUNK), CHUNK)
                mean[unit, at, :] = ring[unit % RING, OWN, at, :].astype(BF16).astype(F32)
                return 0

            lax.fori_loop(0, UNIT_ROWS // CHUNK, rows, 0)

    def add_up(group):
        grad_copies(group).wait_recv()
        wait_weights(group)

        @pl.when(group >= SEND_SLOTS)
        def _():
            wait_mean_out(group - SEND_SLOTS)

        for j in range(PAIR):
            unit = PAIR * group + j

            def rows(i, sums):
                at = pl.ds(pl.multiple_of(i * CHUNK, CHUNK), CHUNK)
                near, far, cross = (recv[k - 1, unit, at, :].astype(F32) for k in OTHERS)
                total = (mean[unit, at, :] + near + (far + cross)) / len(PARTNERS)
                mean[unit, at, :] = total
                weight = held[unit, at, :]
                g_sum, w_sum = sums
                return g_sum + fold(total * total), w_sum + fold(weight * weight)

            g_part, w_part = lax.fori_loop(0, UNIT_ROWS // CHUNK, rows, (zeros(), zeros()))
            n_sum[...] += g_part

            def body(kind, index):
                tensor = LAYERS * kind + index // BLOCKS[kind]
                w_sums[tensor] += w_part

            for_kind(unit, KINDS, body)
            start_mean_out(unit)

    def exchange_step(group, _):
        for j in range(PAIR):
            start_weight(PAIR * group + j)

        @pl.when(group >= SEND_SLOTS)
        def _():
            grad_copies(group - SEND_SLOTS).wait_send()

        convert(group)
        keep_own(group)
        for k in (FAR, CROSS, NEAR):
            grad_copy(group, k).start()

        for j in range(PAIR):
            unit = PAIR * group + j

            @pl.when(unit + RING < UNITS)
            def _():
                start_grads(unit + RING)

            @pl.when(unit + RING >= UNITS)
            def _():
                for other in range(PAIR):
                    start_moments(PAIR * (unit + RING - UNITS) + other, (PROJ, QKV))

        @pl.when(group >= LAG + 1)
        def _():
            add_up(group - LAG - 1)

        return 0

    lax.fori_loop(0, GROUPS, exchange_step, 0)

    def drain_step(group, _):
        add_up(group)
        return 0

    lax.fori_loop(GROUPS - LAG - 1, GROUPS, drain_step, 0)

    n_note, early_note = len(KINDS), len(KINDS) + 1

    def rows_of(index):
        return pl.ds(0, TILE[0] if index in (n_note, early_note) else 1)

    def send_note(index):
        for slot, peer in enumerate(peers):
            pltpu.make_async_remote_copy(
                note.at[index, rows_of(index)], notes.at[index, slot, rows_of(index)], note_sem.at[0, index], note_sem.at[1, index],
                device_id=device(peer), device_id_type=MESH).start()

    def read_note(index):
        arrived = notes.at[index, pl.ds(0, len(peers)), rows_of(index)]
        remote(arrived, arrived, note_sem.at[0, index], note_sem.at[1, index], FAR).wait()
        return note[index] + jnp.sum(notes[index], axis=0)

    note[n_note] = n_sum[...]

    def settle(group, _):
        grad_copies(group).wait_send()
        return 0

    lax.fori_loop(GROUPS - SEND_SLOTS, GROUPS, settle, 0)
    send_note(n_note)

    def settle_means(group, _):
        wait_mean_out(group)
        return 0

    lax.fori_loop(GROUPS - SEND_SLOTS, GROUPS, settle_means, 0)
    total_sq = jnp.sum(jnp.sum(read_note(n_note), axis=0, keepdims=True), axis=1, keepdims=True)
    clip = jnp.minimum(1.0, MAX_NORM / jnp.sqrt(total_sq))
    scal[len(KINDS)] = jnp.broadcast_to(clip, TILE)

    def directions(kind, unit_from, unit_to):
        def group_step(index, _):
            group = FIRST[kind] // PAIR + index
            slot = group % RING
            wait_ring(slot)
            total = zeros()
            for j in range(PAIR):
                unit, part = PAIR * group + j, PAIR * j
                for i in range(0, UNIT_ROWS, CHUNK):
                    at = pl.ds(i, CHUNK)
                    update, _, _ = adam_direction(mean[unit, at, :], held[unit, at, :], ring[slot, part, at, :], ring[slot, part + 1, at, :], clip)
                    mean[unit, at, :] = update
                    total = total + fold(update * update)
            u_sums[LAYERS * kind + PAIR * index // BLOCKS[kind]] += total
            return 0

        lax.fori_loop(unit_from // PAIR, unit_to // PAIR, group_step, 0)

    def refill(unit_from, unit_to):
        def unit_step(unit, _):
            start_moments(unit + RESIDENT, (FCIN, FCOUT))
            return 0

        lax.fori_loop(unit_from, unit_to, unit_step, 0)

    def tensor_sums(kind, layers):
        return [jnp.sum(sums[LAYERS * kind + layer], axis=0, keepdims=True) for sums in (u_sums, w_sums) for layer in range(layers)]

    def write_early_note():
        for row, total in zip((0, LAYERS), tensor_sums(PROJ, 1)):
            note[early_note, row:row + 1, :] = total

    def write_note(kind):
        lane = lax.broadcasted_iota(jnp.int32, (1, TILE[1]), 1)
        packed = jnp.zeros((1, TILE[1]), F32)
        for index, total in enumerate(tensor_sums(kind, LAYERS)):
            packed = jnp.where(lane == index, jnp.sum(total, axis=1, keepdims=True), packed)
        note[kind, :1, :] = packed

    def early_ratio():
        norms = jnp.sqrt(jnp.sum(read_note(early_note), axis=1, keepdims=True))
        scal[PROJ, :1, :] = jnp.broadcast_to(norms[LAYERS:LAYERS + 1] / norms[:1], (1, TILE[1]))

    def ratios(kind):
        norms = jnp.sqrt(read_note(kind)[:1, :])
        for layer in range(LAYERS):
            ratio = norms[:, LAYERS + layer:LAYERS + layer + 1] / norms[:, layer:layer + 1]
            scal[kind, layer:layer + 1, :] = jnp.broadcast_to(ratio, (1, TILE[1]))

    def new_weights(kind, unit_from, unit_to, target):
        def unit_step(index, _):
            unit = FIRST[kind] + index
            ratio = LEARN_RATE * scal[kind, pl.ds(index // BLOCKS[kind], 1), :][:, :1]
            for i in range(0, UNIT_ROWS, CHUNK):
                at = pl.ds(i, CHUNK)
                target[unit, at, :] = (held[unit, at, :] - ratio * mean[unit, at, :]).astype(BF16)
            return 0

        lax.fori_loop(unit_from, unit_to, unit_step, 0)

    near_sem = PAIR * SENT_GROUPS

    def rep_copy(group, k):
        source = recv.at[FAR - 1, pair(group)] if k == CROSS else stage.at[pair(group)]
        arrival = {NEAR: near_sem, FAR: group, CROSS: SENT_GROUPS + group}[k]
        return remote(source, recv.at[k - 1, pair(group)], rep_send_sem.at[k - 1], recv_sem.at[arrival], FAR if k == FAR else NEAR)

    def late_copy(group):
        target = late.at[pair(group - RELAYED)] if group < TAIL_FIRST else tail.at[pair(group - TAIL_FIRST)]
        return remote(stage.at[pair(group)], target, rep_send_sem.at[FAR - 1], recv_sem.at[group], FAR)

    def all_copies(k, count):
        return remote(landed(count), landed(count), rep_send_sem.at[k - 1], recv_sem.at[near_sem], NEAR)

    def start_replicas(unit_from, unit_to):
        def body(group, _):
            rep_copy(group, FAR).start()
            rep_copy(group, NEAR).start()
            return 0

        lax.fori_loop(unit_from // PAIR, unit_to // PAIR, body, 0)

    def start_late_replicas():
        for group in range(RELAYED, SENT_GROUPS):
            if group < TAIL_FIRST:
                late_copy(group).start()
            else:
                pl.when(stays)(late_copy(group).start)
            rep_copy(group, NEAR).start()

    def replicas_out(unit_from, unit_to, k):
        def unit_step(unit, _):
            def body(kind, index):
                source = recv.at[k - 1, unit] if k else stage.at[unit]
                pltpu.make_async_copy(source, unit_at(reps[kind], kind, index, partner[k]), mean_sem.at[k]).start()

            for_kind(unit, (PROJ, QKV), body)
            return 0

        lax.fori_loop(unit_from, unit_to, unit_step, 0)

    def pieces_out(kind):
        for ref, (layer, first, rows) in zip(pieces[kind], PIECES[kind - FCIN]):
            for row in range(0, rows, UNIT_ROWS):
                for column in range(COL_BLOCKS[kind]):
                    unit = FIRST[kind] + layer * BLOCKS[kind] + (first + row) // UNIT_ROWS * COL_BLOCKS[kind] + column
                    target = ref.at[0, pl.ds(row, UNIT_ROWS), pl.ds(column * UNIT_COLS, UNIT_COLS)]
                    pltpu.make_async_copy(recv.at[0, unit], target, mean_sem.at[PAIR + kind]).start()

    proj_end, qkv_end, piece_end = (FIRST[kind + 1] - FIRST[kind] for kind in (PROJ, QKV, FCIN))
    first, half = BLOCKS[PROJ], qkv_end // PAIR
    directions(PROJ, 0, first)
    write_early_note()
    refill(0, first)
    send_note(early_note)
    directions(PROJ, first, proj_end)
    write_note(PROJ)
    directions(QKV, 0, PAIR)
    send_note(PROJ)
    directions(QKV, PAIR, half)
    early_ratio()
    new_weights(PROJ, 0, first, stage)
    refill(first, PAIR * first)
    start_replicas(0, first)
    ratios(PROJ)
    new_weights(PROJ, first, proj_end, stage)
    directions(QKV, half, qkv_end)
    start_replicas(first, PAIR * first)
    write_note(QKV)
    refill(PAIR * first, SENT_UNITS)
    send_note(QKV)
    start_replicas(PAIR * first, proj_end)
    directions(FCIN, 0, piece_end // PAIR)
    ratios(QKV)
    new_weights(QKV, 0, half, stage)
    directions(FCIN, piece_end // PAIR, piece_end // PAIR + PAIR)
    start_replicas(proj_end, proj_end + half // PAIR)
    directions(FCIN, piece_end // PAIR + PAIR, piece_end)
    refill(FIRST[FCIN], FIRST[FCOUT])
    new_weights(QKV, half, qkv_end, stage)
    directions(FCOUT, 0, piece_end)
    write_note(FCIN)
    write_note(FCOUT)
    extra_copy = pltpu.make_async_copy(stage.at[pl.ds(PAIR * TAIL_FIRST, PAIR * TAIL_GROUPS)], extra, mean_sem.at[SEND_SLOTS - 1])
    extra_copy.start()
    send_note(FCIN)
    send_note(FCOUT)
    start_replicas(proj_end + half // PAIR, PAIR * RELAYED)
    start_late_replicas()
    replicas_out(0, SENT_UNITS, OWN)
    for kind in (FCIN, FCOUT):
        ratios(kind)
        new_weights(kind, 0, piece_end, recv.at[0])
    scal_copy = pltpu.make_async_copy(scal, scal_out, mean_sem.at[len(KINDS) + PAIR])
    scal_copy.start()
    pieces_out(FCIN)
    pieces_out(FCOUT)
    all_copies(NEAR, SENT_UNITS).wait()
    replicas_out(0, SENT_UNITS, NEAR)

    def relay_step(group, _):
        @pl.when(group < RELAYED)
        def _():
            rep_copy(group, FAR).wait_recv()
            rep_copy(group, CROSS).start()
            replicas_out(PAIR * group, PAIR * group + PAIR, FAR)

        @pl.when(group >= 1)
        def _():
            rep_copy(group - 1, CROSS).wait_recv()
            replicas_out(PAIR * group - PAIR, PAIR * group, CROSS)

        return 0

    lax.fori_loop(0, RELAYED + 1, relay_step, 0)
    all_copies(CROSS, PAIR * RELAYED).wait_send()
    for index, count in enumerate((SENT_UNITS, SENT_UNITS, PAIR * RELAYED, PAIR * RELAYED, PIECE_UNITS, PIECE_UNITS)):
        pltpu.make_async_copy(landed(count), landed(count), mean_sem.at[index]).wait()
    scal_copy.wait()
    extra_copy.wait()
    for group in range(RELAYED, TAIL_FIRST):
        late_copy(group).wait_recv()

    @pl.when(stays)
    def _():
        all_copies(FAR, SENT_UNITS).wait_send()
        for group in range(TAIL_FIRST, SENT_GROUPS):
            late_copy(group).wait_recv()

    @pl.when(jnp.logical_not(stays))
    def _():
        all_copies(FAR, PAIR * TAIL_FIRST).wait_send()


def place_static(kind, index):
    block = index % BLOCKS[kind]
    return index // BLOCKS[kind], block // COL_BLOCKS[kind] * UNIT_ROWS, block % COL_BLOCKS[kind] * UNIT_COLS


def start_grads_static(unit, grads, ring, ring_sem, partner):
    kind = next(kind for kind in KINDS if unit < FIRST[kind + 1])
    layer, row, col = place_static(kind, unit - FIRST[kind])
    for k in PARTNERS:
        base = pl.multiple_of(partner[k] * SHARD_ROWS[kind] + row, UNIT_ROWS)
        pltpu.make_async_copy(grads[kind].at[0, layer, pl.ds(base, UNIT_ROWS), pl.ds(col, UNIT_COLS)], ring.at[unit, k], ring_sem.at[unit]).start()


def assemble_kernel(*refs):
    (proj, qkv), far_parts, cross_parts, own, near, outs, scratch = split(refs, PAIR, PAIR, PAIR, PIECE_COUNT, PIECE_COUNT, len(KINDS), 7)
    proj_buf, qkv_buf, in_buf, out_buf, late_sem, whole_sem, piece_sem = scratch
    partner = partners(lax.axis_index("data"))
    copies = []

    def through(source, buffer, target, sem):
        copies.append((pltpu.make_async_copy(source, buffer, sem.at[0]), pltpu.make_async_copy(buffer, target, sem.at[1])))

    for layer in range(LAYERS):
        through(qkv.at[layer], qkv_buf.at[layer], outs[QKV].at[layer], whole_sem.at[layer])
    through(proj, proj_buf, outs[PROJ], whole_sem.at[LAYERS])
    order = [(kind, piece) for kind in (FCIN, FCOUT) for piece in PIECES[kind - FCIN]]
    for number, (kind, (layer, first, rows)) in enumerate(order):
        for k, piece in ((OWN, own[number]), (NEAR, near[number])):
            at = (in_buf if kind == FCIN else out_buf).at[k, pl.ds(layer, 1), pl.ds(first, rows)]
            base = pl.multiple_of(partner[k] * SHARD_ROWS[kind] + first, UNIT_ROWS)
            through(piece, at, outs[kind].at[pl.ds(layer, 1), pl.ds(base, rows)], piece_sem.at[k, number])
    fills = [[] for _ in range(LAYERS)]
    for k, sources in ((FAR, far_parts), (CROSS, cross_parts)):
        units = [source.at[unit] for source in sources for unit in range(source.shape[0])]
        for number, source in enumerate(units):
            layer, row, col = place_static(QKV, PAIR * RELAYED + number - FIRST[QKV])
            base = pl.multiple_of(partner[k] * SHARD_ROWS[QKV] + row, UNIT_ROWS)
            target = qkv_buf.at[layer, pl.ds(base, UNIT_ROWS), pl.ds(col, UNIT_COLS)]
            fills[layer].append(pltpu.make_async_copy(source, target, late_sem.at[k - FAR, number]))
    for fetch, _ in copies:
        fetch.start()
    for (fetch, _), layer_fills in zip(copies, fills):
        fetch.wait()
        for fill in layer_fills:
            fill.start()
    for (_, store), layer_fills in zip(copies, fills):
        for fill in layer_fills:
            fill.wait()
        store.start()
    for fetch, store in copies[LAYERS:]:
        fetch.wait()
        store.start()
    for _, store in copies:
        store.wait()


def assemble(reps, far_parts, cross_parts, own, near):
    shape, dma = jax.ShapeDtypeStruct, pltpu.SemaphoreType.DMA
    whole = [(LAYERS, len(PARTNERS) * rows, cols) for rows, cols in zip(SHARD_ROWS, SHARD_COLS)]
    any_spec = pl.BlockSpec(memory_space=pl.ANY)
    operands = [*reps, *far_parts, *cross_parts, *own, *near]
    return pl.pallas_call(
        assemble_kernel,
        out_shape=[shape(s, BF16) for s in whole],
        in_specs=[any_spec] * len(operands),
        out_specs=[any_spec] * len(whole),
        scratch_shapes=[
            pltpu.VMEM(whole[PROJ], BF16),
            pltpu.VMEM(whole[QKV], BF16),
            pltpu.VMEM((PAIR, LAYERS, SHARD_ROWS[FCIN], SHARD_COLS[FCIN]), BF16),
            pltpu.VMEM((PAIR, LAYERS, SHARD_ROWS[FCOUT], SHARD_COLS[FCOUT]), BF16),
            dma((PAIR, SENT_UNITS - PAIR * RELAYED)), dma((LAYERS + 1, PAIR)), dma((PAIR, len(own), PAIR)),
        ],
        compiler_params=pltpu.CompilerParams(vmem_limit_bytes=24_000_000),
        cost_estimate=pl.CostEstimate(flops=12_000_000, bytes_accessed=38_000_000, transcendentals=0),
    )(*operands)


def solution(mesh):
    in_specs = []
    for col_split in COLUMN_SPLIT:
        in_specs.extend([grad_spec(col_split), state_spec(col_split), state_spec(col_split), state_spec(col_split)])
    out_specs = tuple([replica_spec(col_split) for col_split in COLUMN_SPLIT] + [state_spec(col_split) for col_split in COLUMN_SPLIT] * 3)
    across, beside = ([(i, partners(i)[k]) for i in PARTNERS] for k in (FAR, NEAR))
    leavers = [(i, k) for i, k in across if i % PAIR == 0]

    def device_step(*arrays):
        shape = jax.ShapeDtypeStruct
        shard = [(LAYERS, rows, cols) for rows, cols in zip(SHARD_ROWS, SHARD_COLS)]
        order = [(kind, piece) for kind in (FCIN, FCOUT) for piece in PIECES[kind - FCIN]]
        scal_shape = (len(KINDS) + 1,) + TILE
        unit = (UNIT_ROWS, UNIT_COLS)
        out_shape = (
            [shape(s, F32) for s in shard]
            + [shape((LAYERS, len(PARTNERS) * SHARD_ROWS[kind], SHARD_COLS[kind]), BF16) for kind in (PROJ, QKV)]
            + [shape((1, rows, SHARD_COLS[kind]), BF16) for kind, (_, _, rows) in order]
            + [shape((PAIR * count,) + unit, BF16) for count in (LATE_GROUPS, TAIL_GROUPS, TAIL_GROUPS)] + [shape(scal_shape, F32)])
        any_spec = pl.BlockSpec(memory_space=pl.ANY)
        dma = pltpu.SemaphoreType.DMA
        messages = len(KINDS) + PAIR
        operands = [arrays[len(KINDS) * kind + part] for part in PARTNERS for kind in KIND_ORDER]
        results = pl.pallas_call(
            step_kernel,
            out_shape=out_shape,
            in_specs=[any_spec] * len(operands),
            out_specs=[any_spec] * len(out_shape),
            scratch_shapes=[
                pltpu.VMEM((len(OTHERS), UNITS) + unit, BF16),
                pltpu.VMEM((len(OTHERS) * PAIR * SEND_SLOTS,) + unit, BF16),
                pltpu.VMEM((UNITS,) + unit, F32),
                pltpu.VMEM((UNITS,) + unit, F32),
                pltpu.VMEM((RING, len(PARTNERS)) + unit, F32),
                pltpu.VMEM((messages,) + TILE, F32),
                pltpu.VMEM((messages, mesh.size - 1) + TILE, F32),
                pltpu.VMEM((LAYERS * len(KINDS),) + TILE, F32),
                pltpu.VMEM((LAYERS * len(KINDS),) + TILE, F32),
                pltpu.VMEM(TILE, F32),
                pltpu.VMEM(scal_shape, F32),
                dma((RING,)), dma((RING,)), dma((SEND_SLOTS,)), dma((SEND_SLOTS,)), dma((GROUPS,)), dma((len(OTHERS),)), dma((PAIR, messages)),
            ],
            compiler_params=pltpu.CompilerParams(collective_id=0, has_side_effects=True, vmem_limit_bytes=66_900_000),
        )(*operands)
        means, reps, pieces, (late, tail, extra, scal) = split(results, len(KINDS), PAIR, PIECE_COUNT, 4)
        data = lax.axis_index("data")
        owners = partners(data)
        state = {}
        clip = scal[len(KINDS), 0, 0]
        for slot, kind in enumerate(KIND_ORDER):
            _, weight, moment1, moment2 = arrays[len(KINDS) * kind:len(KINDS) * kind + len(KINDS)]
            update, new_first, new_second = adam_direction(means[slot], weight, moment1, moment2, clip)
            ratio = jnp.expand_dims(scal[slot, :LAYERS, 0], (1, 2))
            state[kind] = (weight - LEARN_RATE * ratio * update, new_first, new_second)
        far, near = [], []
        for piece in pieces:
            far.append(lax.ppermute(piece, "data", across))
        arrived = lax.ppermute(extra, "data", leavers)
        far_parts = (late, jnp.where(data % PAIR == 0, arrived, tail))
        cross_parts = [lax.ppermute(part, "data", beside) for part in far_parts]
        near = [lax.ppermute(piece, "data", beside) for piece in pieces]
        replicas = list(assemble(reps, far_parts, cross_parts, pieces, near))
        for number, (kind, (layer, first, _)) in enumerate(order):
            far_near = lax.ppermute(far[number], "data", beside)
            for piece, k in ((far[number], FAR), (far_near, CROSS)):
                replicas[kind] = lax.dynamic_update_slice(replicas[kind], piece, (layer, owners[k] * SHARD_ROWS[kind] + first, 0))
        outputs = [replicas[KIND_ORDER.index(kind)] for kind in KINDS]
        return tuple(outputs + [state[kind][part] for part in range(len(OTHERS)) for kind in KINDS])

    return jax.shard_map(device_step, mesh=mesh, in_specs=tuple(in_specs), out_specs=out_specs, check_vma=False)
```

```python
import functools

import jax
import jax.numpy as jnp
from jax import lax
from jax.experimental import pallas as pl
from jax.experimental.pallas import tpu as pltpu
from jax.sharding import PartitionSpec as P


LEARN_RATE = 0.08
BETA_ONE = 0.9
BETA_TWO = 0.999
ADAM_EPS = 1e-6
DECAY_RATE = 0.01
MAX_NORM = 1.0
STEP_COUNT = 100
COLUMN_SPLIT = (True, False, True, False)
MESH = pl.DeviceIdType.MESH
F32, BF16 = jnp.float32, jnp.bfloat16

UNIT_ROWS, UNIT_COLS = 96, 384
CHUNK = 16
PAIR = 2
TILE = (8, 128)
OWN, NEAR, FAR, CROSS = PARTNERS = range(4)
OTHERS = (NEAR, FAR, CROSS)
PROJ, QKV, FCIN, FCOUT = KINDS = range(4)
KIND_ORDER = (1, 0, 2, 3)
SHARD_ROWS = (96, 192, 192, 384)
SHARD_COLS = (768, 1152, 1536, 768)
LAYERS = 4
COL_BLOCKS = tuple(cols // UNIT_COLS for cols in SHARD_COLS)
BLOCKS = tuple(rows // UNIT_ROWS * (cols // UNIT_COLS) for rows, cols in zip(SHARD_ROWS, SHARD_COLS))
FIRST = tuple(sum(LAYERS * blocks for blocks in BLOCKS[:k]) for k in range(5))
UNITS = FIRST[-1]
GROUPS = UNITS // PAIR
RING = 16
SEND_SLOTS = 8
LAG = 8
RESIDENT = PAIR * RING
SENT_UNITS = FIRST[FCIN]
SENT_GROUPS = SENT_UNITS // PAIR
PIECE_UNITS = FIRST[FCOUT] - FIRST[FCIN]
LATE_GROUPS = 2
TAIL_GROUPS = 5
TAIL_FIRST = SENT_GROUPS - TAIL_GROUPS
RELAYED = TAIL_FIRST - LATE_GROUPS
AHEAD = 1
LAST_ROWS = 192
PIECES = tuple(
    [(layer, 0, SHARD_ROWS[kind]) for layer in range(LAYERS - (kind == FCOUT))]
    + [(LAYERS - 1, 0, SHARD_ROWS[kind] - LAST_ROWS), (LAYERS - 1, SHARD_ROWS[kind] - LAST_ROWS, LAST_ROWS)] * (kind == FCOUT)
    for kind in (FCIN, FCOUT))
PIECE_COUNT = sum(map(len, PIECES))


def grad_spec(col_split):
    return P("data", None, None, "model") if col_split else P("data", None, "model", None)


def state_spec(col_split):
    return P(None, "data", "model") if col_split else P(None, ("model", "data"), None)


def replica_spec(col_split):
    return P(None, None, "model") if col_split else P(None, "model", None)


def adam_direction(grad_mean, weight, moment1, moment2, clip_coef):
    clipped = clip_coef * grad_mean
    new_first = BETA_ONE * moment1 + (1.0 - BETA_ONE) * clipped
    new_second = BETA_TWO * moment2 + (1.0 - BETA_TWO) * clipped * clipped
    first_hat = new_first / (1.0 - BETA_ONE ** STEP_COUNT)
    second_hat = new_second / (1.0 - BETA_TWO ** STEP_COUNT)
    update = first_hat / (jnp.sqrt(second_hat) + ADAM_EPS) + DECAY_RATE * weight
    return update, new_first, new_second


def fold(x):
    sublanes, lanes = TILE
    parts = [x[i:i + sublanes, j:j + lanes] for i in range(0, CHUNK, sublanes) for j in range(0, UNIT_COLS, lanes)]
    return functools.reduce(jnp.add, parts)


def pair(group):
    return pl.ds(PAIR * group, PAIR)


def partners(data):
    return data, data + 1 - PAIR * (data % PAIR), (data + PAIR) % len(PARTNERS), CROSS - data


def zeros():
    return jnp.zeros(TILE, F32)


def split(items, *counts):
    items = iter(items)
    return [[next(items) for _ in range(count)] for count in counts]


def place(kind, index):
    blocks, col_blocks = BLOCKS[kind], COL_BLOCKS[kind]
    layer, block = index // blocks, index % blocks
    row = pl.multiple_of(block // col_blocks * UNIT_ROWS, UNIT_ROWS)
    col = pl.multiple_of(block % col_blocks * UNIT_COLS, UNIT_COLS)
    return layer, row, col


def for_kind(unit, kinds, body):
    for kind in kinds:
        @pl.when((unit >= FIRST[kind]) & (unit < FIRST[kind + 1]))
        def _():
            body(kind, unit - FIRST[kind])


def step_kernel(*refs):
    counts = tuple(map(len, PIECES))
    grads, weights, firsts, seconds, means, reps, in_pieces, out_pieces, rest = split(refs, *[len(KINDS)] * 5, PAIR, *counts, 23)
    pieces = {FCIN: in_pieces, FCOUT: out_pieces}
    (late, tail, extra, scal_out, recv, ahead, stage, mean, held, ring, note, notes, w_sums, u_sums, n_sum, scal,
     ring_sem, held_sem, mean_sem, send_sem, recv_sem, rep_send_sem, note_sem) = rest
    model, data = lax.axis_index("model"), lax.axis_index("data")
    partner = partners(data)
    stays = data % PAIR == 1

    def unit_at(ref, kind, index, quarter_base=None):
        layer, row, col = place(kind, index)
        if quarter_base is not None:
            row = pl.multiple_of(quarter_base * SHARD_ROWS[kind] + row, UNIT_ROWS)
            return ref.at[layer, pl.ds(row, UNIT_ROWS), pl.ds(col, UNIT_COLS)]
        return ref.at[layer, pl.ds(row, UNIT_ROWS), pl.ds(col, UNIT_COLS)]

    def start_grads(unit):
        def body(kind, index):
            for k in PARTNERS:
                pltpu.make_async_copy(unit_at(grads[kind].at[0], kind, index, partner[k]), ring.at[unit % RING, k], ring_sem.at[unit % RING]).start()

        for_kind(unit, KINDS, body)

    def start_moments(unit, kinds):
        slot, part = unit // PAIR % RING, PAIR * (unit % PAIR)

        def body(kind, index):
            pltpu.make_async_copy(unit_at(firsts[kind], kind, index), ring.at[slot, part], ring_sem.at[slot]).start()
            pltpu.make_async_copy(unit_at(seconds[kind], kind, index), ring.at[slot, part + 1], ring_sem.at[slot]).start()

        for_kind(unit, kinds, body)

    def start_weight(unit):
        def body(kind, index):
            pltpu.make_async_copy(unit_at(weights[kind], kind, index), held.at[unit], held_sem.at[unit // PAIR % RING]).start()

        for_kind(unit, KINDS, body)

    def start_mean_out(unit):
        def body(kind, index):
            pltpu.make_async_copy(mean.at[unit], unit_at(means[kind], kind, index), mean_sem.at[unit // PAIR % SEND_SLOTS]).start()

        for_kind(unit, KINDS, body)

    def block(ref, count):
        return ref.at[pl.ds(0, count), pl.ds(0, UNIT_ROWS), pl.ds(0, UNIT_COLS)]

    def wait_ring(slot):
        pltpu.make_async_copy(block(grads[QKV].at[0], len(PARTNERS)), ring.at[slot], ring_sem.at[slot]).wait()

    def wait_weights(group):
        pltpu.make_async_copy(block(weights[QKV], PAIR), held.at[pair(group)], held_sem.at[group % RING]).wait()

    def wait_mean_out(group):
        pltpu.make_async_copy(mean.at[pair(group)], block(means[QKV], PAIR), mean_sem.at[group % SEND_SLOTS]).wait()

    def landed(count):
        return recv.at[0, pl.ds(0, count)]

    def remote(source, target, sent, received, k):
        return pltpu.make_async_remote_copy(source, target, sent, received, device_id=(model, partner[k]), device_id_type=MESH)

    def stage_slot(group, k):
        return group % SEND_SLOTS * len(OTHERS) + k - 1

    def grad_copy(group, k):
        return remote(stage.at[pair(stage_slot(group, k))], recv.at[k - 1, pair(group)], send_sem.at[group % SEND_SLOTS], recv_sem.at[group], k)

    def grad_copies(group):
        count = len(OTHERS) * PAIR
        return remote(landed(count), landed(count), send_sem.at[group % SEND_SLOTS], recv_sem.at[group], FAR)

    early = PAIR
    for unit in range(early):
        start_grads_static(unit, grads, ring, ring_sem, partner)

    barrier = pltpu.get_barrier_semaphore()
    peers = [(side, k) for k in (FAR, CROSS, OWN, NEAR) for side in (1, 0) if side or k]

    def device(peer):
        return (model + peer[0]) % PAIR, partner[peer[1]]

    for peer in peers:
        pl.semaphore_signal(barrier, inc=1, device_id=device(peer), device_id_type=MESH)
    for unit in range(early, RING):
        start_grads_static(unit, grads, ring, ring_sem, partner)

    n_sum[...] = jnp.zeros_like(n_sum)
    note[...] = jnp.zeros_like(note)
    w_sums[...] = jnp.zeros_like(w_sums)
    u_sums[...] = jnp.zeros_like(u_sums)

    def convert(group):
        for j in range(PAIR):
            unit = PAIR * group + j
            wait_ring(unit % RING)

            def rows(i, _):
                at = pl.ds(pl.multiple_of(i * CHUNK, CHUNK), CHUNK)
                for k in OTHERS:
                    stage[PAIR * stage_slot(group, k) + j, at, :] = ring[unit % RING, k, at, :].astype(BF16)
                return 0

            lax.fori_loop(0, UNIT_ROWS // CHUNK, rows, 0)

    def keep_own(group):
        for j in range(PAIR):
            unit = PAIR * group + j

            def rows(i, _):
                at = pl.ds(pl.multiple_of(i * CHUNK, CHUNK), CHUNK)
                mean[unit, at, :] = ring[unit % RING, OWN, at, :].astype(BF16).astype(F32)
                return 0

            lax.fori_loop(0, UNIT_ROWS // CHUNK, rows, 0)

    def add_up(group):
        grad_copies(group).wait_recv()
        wait_weights(group)

        @pl.when(group >= SEND_SLOTS)
        def _():
            wait_mean_out(group - SEND_SLOTS)

        for j in range(PAIR):
            unit = PAIR * group + j

            def rows(i, sums):
                at = pl.ds(pl.multiple_of(i * CHUNK, CHUNK), CHUNK)
                near, far, cross = (recv[k - 1, unit, at, :].astype(F32) for k in OTHERS)
                total = (mean[unit, at, :] + near + (far + cross)) / len(PARTNERS)
                mean[unit, at, :] = total
                weight = held[unit, at, :]
                g_sum, w_sum = sums
                return g_sum + fold(total * total), w_sum + fold(weight * weight)

            g_part, w_part = lax.fori_loop(0, UNIT_ROWS // CHUNK, rows, (zeros(), zeros()))
            n_sum[...] += g_part

            def body(kind, index):
                tensor = LAYERS * kind + index // BLOCKS[kind]
                w_sums[tensor] += w_part

            for_kind(unit, KINDS, body)
            start_mean_out(unit)

    convert(0)
    keep_own(0)
    pl.semaphore_wait(barrier, len(peers))

    def exchange_step(group, _):
        for j in range(PAIR):
            start_weight(PAIR * group + j)

        @pl.when(group >= SEND_SLOTS)
        def _():
            grad_copies(group - SEND_SLOTS).wait_send()

        @pl.when(group >= 1)
        def _():
            convert(group)
            keep_own(group)

        for k in (FAR, CROSS, NEAR):
            grad_copy(group, k).start()

        for j in range(PAIR):
            unit = PAIR * group + j

            @pl.when(unit + RING < UNITS)
            def _():
                start_grads(unit + RING)

            @pl.when(unit + RING >= UNITS)
            def _():
                for other in range(PAIR):
                    start_moments(PAIR * (unit + RING - UNITS) + other, (PROJ, QKV))

        @pl.when(group >= LAG + 1)
        def _():
            add_up(group - LAG - 1)

        return 0

    lax.fori_loop(0, GROUPS, exchange_step, 0)

    def drain_step(group, _):
        add_up(group)
        return 0

    lax.fori_loop(GROUPS - LAG - 1, GROUPS, drain_step, 0)

    n_note, early_note = len(KINDS), len(KINDS) + 1

    def rows_of(index):
        return pl.ds(0, TILE[0] if index in (n_note, early_note) else 1)

    def send_note(index):
        for slot, peer in enumerate(peers):
            pltpu.make_async_remote_copy(
                note.at[index, rows_of(index)], notes.at[index, slot, rows_of(index)], note_sem.at[0, index], note_sem.at[1, index],
                device_id=device(peer), device_id_type=MESH).start()

    def read_note(index):
        arrived = notes.at[index, pl.ds(0, len(peers)), rows_of(index)]
        remote(arrived, arrived, note_sem.at[0, index], note_sem.at[1, index], FAR).wait()
        return note[index] + jnp.sum(notes[index], axis=0)

    def ahead_copy(part, first_row=0, end_row=UNIT_ROWS):
        rows, sem = pl.ds(first_row, end_row - first_row), len(KINDS) + PAIR + part
        return remote((held, mean)[part].at[AHEAD, rows], ahead.at[part, rows], note_sem.at[0, sem], note_sem.at[1, sem], FAR)

    note[n_note] = n_sum[...]

    def settle(group, _):
        grad_copies(group).wait_send()
        return 0

    lax.fori_loop(GROUPS - SEND_SLOTS, GROUPS, settle, 0)
    send_note(n_note)
    ahead_copy(0).start()

    def settle_means(group, _):
        wait_mean_out(group)
        return 0

    lax.fori_loop(GROUPS - SEND_SLOTS, GROUPS, settle_means, 0)
    total_sq = jnp.sum(jnp.sum(read_note(n_note), axis=0, keepdims=True), axis=1, keepdims=True)
    clip = jnp.minimum(1.0, MAX_NORM / jnp.sqrt(total_sq))
    scal[len(KINDS)] = jnp.broadcast_to(clip, TILE)

    def directions(kind, unit_from, unit_to):
        def group_step(index, _):
            group = FIRST[kind] // PAIR + index
            slot = group % RING
            wait_ring(slot)
            total = zeros()
            for j in range(PAIR):
                unit, part = PAIR * group + j, PAIR * j
                for i in range(0, UNIT_ROWS, CHUNK):
                    at = pl.ds(i, CHUNK)
                    update, _, _ = adam_direction(mean[unit, at, :], held[unit, at, :], ring[slot, part, at, :], ring[slot, part + 1, at, :], clip)
                    mean[unit, at, :] = update
                    total = total + fold(update * update)
            u_sums[LAYERS * kind + PAIR * index // BLOCKS[kind]] += total
            return 0

        lax.fori_loop(unit_from // PAIR, unit_to // PAIR, group_step, 0)

    def refill(unit_from, unit_to):
        def unit_step(unit, _):
            start_moments(unit + RESIDENT, (FCIN, FCOUT))
            return 0

        lax.fori_loop(unit_from, unit_to, unit_step, 0)

    def tensor_sums(kind, layers):
        return [jnp.sum(sums[LAYERS * kind + layer], axis=0, keepdims=True) for sums in (u_sums, w_sums) for layer in range(layers)]

    def write_early_note():
        for row, total in zip((0, LAYERS), tensor_sums(PROJ, 1)):
            note[early_note, row:row + 1, :] = total

    def write_note(kind):
        lane = lax.broadcasted_iota(jnp.int32, (1, TILE[1]), 1)
        packed = jnp.zeros((1, TILE[1]), F32)
        for index, total in enumerate(tensor_sums(kind, LAYERS)):
            packed = jnp.where(lane == index, jnp.sum(total, axis=1, keepdims=True), packed)
        note[kind, :1, :] = packed

    def early_ratio():
        norms = jnp.sqrt(jnp.sum(read_note(early_note), axis=1, keepdims=True))
        scal[PROJ, :1, :] = jnp.broadcast_to(norms[LAYERS:LAYERS + 1] / norms[:1], (1, TILE[1]))

    def ratios(kind):
        norms = jnp.sqrt(read_note(kind)[:1, :])
        for layer in range(LAYERS):
            ratio = norms[:, LAYERS + layer:LAYERS + layer + 1] / norms[:, layer:layer + 1]
            scal[kind, layer:layer + 1, :] = jnp.broadcast_to(ratio, (1, TILE[1]))

    def new_weights(kind, unit_from, unit_to, target):
        def unit_step(index, _):
            unit = FIRST[kind] + index
            ratio = LEARN_RATE * scal[kind, pl.ds(index // BLOCKS[kind], 1), :][:, :1]
            for i in range(0, UNIT_ROWS, CHUNK):
                at = pl.ds(i, CHUNK)
                target[unit, at, :] = (held[unit, at, :] - ratio * mean[unit, at, :]).astype(BF16)
            return 0

        lax.fori_loop(unit_from, unit_to, unit_step, 0)

    def weights_ahead():
        ratio = LEARN_RATE * scal[PROJ, AHEAD // BLOCKS[PROJ]:AHEAD // BLOCKS[PROJ] + 1, :][:, :1]
        for i in range(0, UNIT_ROWS, CHUNK):
            at = pl.ds(i, CHUNK)
            recv[FAR - 1, AHEAD, at, :] = (ahead[0, at, :] - ratio * ahead[1, at, :]).astype(BF16)

    near_sem = PAIR * SENT_GROUPS

    def rep_copy(group, k):
        source = recv.at[FAR - 1, pair(group)] if k == CROSS else stage.at[pair(group)]
        arrival = {NEAR: near_sem, FAR: group, CROSS: SENT_GROUPS + group}[k]
        return remote(source, recv.at[k - 1, pair(group)], rep_send_sem.at[k - 1], recv_sem.at[arrival], FAR if k == FAR else NEAR)

    def first_copy():
        return remote(stage.at[0], recv.at[FAR - 1, 0], rep_send_sem.at[FAR - 1], recv_sem.at[0], FAR)

    def late_copy(group):
        target = late.at[pair(group - RELAYED)] if group < TAIL_FIRST else tail.at[pair(group - TAIL_FIRST)]
        return remote(stage.at[pair(group)], target, rep_send_sem.at[FAR - 1], recv_sem.at[group], FAR)

    def all_copies(k, count):
        return remote(landed(count), landed(count), rep_send_sem.at[k - 1], recv_sem.at[near_sem], NEAR)

    def start_replicas(unit_from, unit_to):
        def body(group, _):
            rep_copy(group, FAR).start()
            rep_copy(group, NEAR).start()
            return 0

        lax.fori_loop(unit_from // PAIR, unit_to // PAIR, body, 0)

    def start_late_replicas():
        for group in range(RELAYED, SENT_GROUPS):
            if group < TAIL_FIRST:
                late_copy(group).start()
            else:
                pl.when(stays)(late_copy(group).start)
            rep_copy(group, NEAR).start()

    def replicas_out(unit_from, unit_to, k):
        def unit_step(unit, _):
            def body(kind, index):
                source = recv.at[k - 1, unit] if k else stage.at[unit]
                pltpu.make_async_copy(source, unit_at(reps[kind], kind, index, partner[k]), mean_sem.at[k]).start()

            for_kind(unit, (PROJ, QKV), body)
            return 0

        lax.fori_loop(unit_from, unit_to, unit_step, 0)

    def pieces_out(kind):
        for ref, (layer, first, rows) in zip(pieces[kind], PIECES[kind - FCIN]):
            for row in range(0, rows, UNIT_ROWS):
                for column in range(COL_BLOCKS[kind]):
                    unit = FIRST[kind] + layer * BLOCKS[kind] + (first + row) // UNIT_ROWS * COL_BLOCKS[kind] + column
                    target = ref.at[0, pl.ds(row, UNIT_ROWS), pl.ds(column * UNIT_COLS, UNIT_COLS)]
                    pltpu.make_async_copy(recv.at[0, unit], target, mean_sem.at[PAIR + kind]).start()

    proj_end, qkv_end, piece_end = (FIRST[kind + 1] - FIRST[kind] for kind in (PROJ, QKV, FCIN))
    first, half = BLOCKS[PROJ], qkv_end // PAIR
    directions(PROJ, 0, first)
    write_early_note()
    refill(0, first)
    send_note(early_note)
    ahead_copy(1, 0, CHUNK * PAIR).start()
    directions(PROJ, first, proj_end)
    write_note(PROJ)
    refill(first, PAIR * first)
    send_note(PROJ)
    ahead_copy(1, CHUNK * PAIR).start()
    directions(QKV, 0, half)
    early_ratio()
    new_weights(PROJ, 0, first, stage)
    refill(PAIR * first, PAIR * first + PAIR)
    first_copy().start()
    rep_copy(0, NEAR).start()
    ratios(PROJ)
    new_weights(PROJ, first, proj_end, stage)
    refill(PAIR * first + PAIR, proj_end)
    start_replicas(first, PAIR * first)
    directions(QKV, half, qkv_end)
    write_note(QKV)
    refill(proj_end, proj_end + PAIR)
    send_note(QKV)
    refill(proj_end + PAIR, SENT_UNITS)
    start_replicas(PAIR * first, proj_end)
    directions(FCIN, 0, piece_end // PAIR)
    ratios(QKV)
    new_weights(QKV, 0, half, stage)
    directions(FCIN, piece_end // PAIR, piece_end // PAIR + PAIR)
    start_replicas(proj_end, proj_end + half // PAIR)
    directions(FCIN, piece_end // PAIR + PAIR, piece_end)
    refill(FIRST[FCIN], FIRST[FCOUT])
    new_weights(QKV, half, qkv_end, stage)
    directions(FCOUT, 0, piece_end)
    write_note(FCIN)
    write_note(FCOUT)
    extra_copy = pltpu.make_async_copy(stage.at[pl.ds(PAIR * TAIL_FIRST, PAIR * TAIL_GROUPS)], extra, mean_sem.at[SEND_SLOTS - 1])
    extra_copy.start()
    send_note(FCIN)
    send_note(FCOUT)
    start_replicas(proj_end + half // PAIR, PAIR * RELAYED)
    start_late_replicas()
    for part in range(PAIR):
        ahead_copy(part).wait()
    weights_ahead()
    replicas_out(0, SENT_UNITS, OWN)
    for kind in (FCIN, FCOUT):
        ratios(kind)
        new_weights(kind, 0, piece_end, recv.at[0])
    scal_copy = pltpu.make_async_copy(scal, scal_out, mean_sem.at[len(KINDS) + PAIR])
    scal_copy.start()
    pieces_out(FCIN)
    pieces_out(FCOUT)
    all_copies(NEAR, SENT_UNITS).wait()
    replicas_out(0, SENT_UNITS, NEAR)

    def relay_step(group, _):
        @pl.when(group < RELAYED)
        def _():
            @pl.when(group == 0)
            def _():
                first_copy().wait_recv()

            @pl.when(group >= 1)
            def _():
                rep_copy(group, FAR).wait_recv()

            rep_copy(group, CROSS).start()
            replicas_out(PAIR * group, PAIR * group + PAIR, FAR)

        @pl.when(group >= 1)
        def _():
            rep_copy(group - 1, CROSS).wait_recv()
            replicas_out(PAIR * group - PAIR, PAIR * group, CROSS)

        return 0

    lax.fori_loop(0, RELAYED + 1, relay_step, 0)
    all_copies(CROSS, PAIR * RELAYED).wait_send()
    for index, count in enumerate((SENT_UNITS, SENT_UNITS, PAIR * RELAYED, PAIR * RELAYED, PIECE_UNITS, PIECE_UNITS)):
        pltpu.make_async_copy(landed(count), landed(count), mean_sem.at[index]).wait()
    scal_copy.wait()
    extra_copy.wait()
    for group in range(RELAYED, TAIL_FIRST):
        late_copy(group).wait_recv()

    @pl.when(stays)
    def _():
        all_copies(FAR, SENT_UNITS - 1).wait_send()
        for group in range(TAIL_FIRST, SENT_GROUPS):
            late_copy(group).wait_recv()

    @pl.when(jnp.logical_not(stays))
    def _():
        all_copies(FAR, PAIR * TAIL_FIRST - 1).wait_send()


def place_static(kind, index):
    block = index % BLOCKS[kind]
    return index // BLOCKS[kind], block // COL_BLOCKS[kind] * UNIT_ROWS, block % COL_BLOCKS[kind] * UNIT_COLS


def start_grads_static(unit, grads, ring, ring_sem, partner):
    kind = next(kind for kind in KINDS if unit < FIRST[kind + 1])
    layer, row, col = place_static(kind, unit - FIRST[kind])
    for k in (FAR, CROSS, NEAR, OWN):
        base = pl.multiple_of(partner[k] * SHARD_ROWS[kind] + row, UNIT_ROWS)
        pltpu.make_async_copy(grads[kind].at[0, layer, pl.ds(base, UNIT_ROWS), pl.ds(col, UNIT_COLS)], ring.at[unit, k], ring_sem.at[unit]).start()


def assemble_kernel(*refs):
    (proj, qkv), far_parts, cross_parts, own, near, outs, scratch = split(refs, PAIR, PAIR, PAIR, PIECE_COUNT, PIECE_COUNT, len(KINDS), 7)
    proj_buf, qkv_buf, in_buf, out_buf, late_sem, whole_sem, piece_sem = scratch
    partner = partners(lax.axis_index("data"))
    copies = []

    def through(source, buffer, target, sem):
        copies.append((pltpu.make_async_copy(source, buffer, sem.at[0]), pltpu.make_async_copy(buffer, target, sem.at[1])))

    for layer in range(LAYERS):
        through(qkv.at[layer], qkv_buf.at[layer], outs[QKV].at[layer], whole_sem.at[layer])
    through(proj, proj_buf, outs[PROJ], whole_sem.at[LAYERS])
    order = [(kind, piece) for kind in (FCIN, FCOUT) for piece in PIECES[kind - FCIN]]
    for number, (kind, (layer, first, rows)) in enumerate(order):
        for k, piece in ((OWN, own[number]), (NEAR, near[number])):
            at = (in_buf if kind == FCIN else out_buf).at[k, pl.ds(layer, 1), pl.ds(first, rows)]
            base = pl.multiple_of(partner[k] * SHARD_ROWS[kind] + first, UNIT_ROWS)
            through(piece, at, outs[kind].at[pl.ds(layer, 1), pl.ds(base, rows)], piece_sem.at[k, number])
    fills = [[] for _ in range(LAYERS)]
    for k, sources in ((FAR, far_parts), (CROSS, cross_parts)):
        units = [source.at[unit] for source in sources for unit in range(source.shape[0])]
        for number, source in enumerate(units):
            layer, row, col = place_static(QKV, PAIR * RELAYED + number - FIRST[QKV])
            base = pl.multiple_of(partner[k] * SHARD_ROWS[QKV] + row, UNIT_ROWS)
            target = qkv_buf.at[layer, pl.ds(base, UNIT_ROWS), pl.ds(col, UNIT_COLS)]
            fills[layer].append(pltpu.make_async_copy(source, target, late_sem.at[k - FAR, number]))
    for fetch, _ in copies:
        fetch.start()
    for (fetch, _), layer_fills in zip(copies, fills):
        fetch.wait()
        for fill in layer_fills:
            fill.start()
    for (_, store), layer_fills in zip(copies, fills):
        for fill in layer_fills:
            fill.wait()
        store.start()
    for fetch, store in copies[LAYERS:]:
        fetch.wait()
        store.start()
    for _, store in copies:
        store.wait()


def assemble(reps, far_parts, cross_parts, own, near):
    shape, dma = jax.ShapeDtypeStruct, pltpu.SemaphoreType.DMA
    whole = [(LAYERS, len(PARTNERS) * rows, cols) for rows, cols in zip(SHARD_ROWS, SHARD_COLS)]
    any_spec = pl.BlockSpec(memory_space=pl.ANY)
    operands = [*reps, *far_parts, *cross_parts, *own, *near]
    return pl.pallas_call(
        assemble_kernel,
        out_shape=[shape(s, BF16) for s in whole],
        in_specs=[any_spec] * len(operands),
        out_specs=[any_spec] * len(whole),
        scratch_shapes=[
            pltpu.VMEM(whole[PROJ], BF16),
            pltpu.VMEM(whole[QKV], BF16),
            pltpu.VMEM((PAIR, LAYERS, SHARD_ROWS[FCIN], SHARD_COLS[FCIN]), BF16),
            pltpu.VMEM((PAIR, LAYERS, SHARD_ROWS[FCOUT], SHARD_COLS[FCOUT]), BF16),
            dma((PAIR, SENT_UNITS - PAIR * RELAYED)), dma((LAYERS + 1, PAIR)), dma((PAIR, len(own), PAIR)),
        ],
        compiler_params=pltpu.CompilerParams(vmem_limit_bytes=24_000_000),
        cost_estimate=pl.CostEstimate(flops=12_000_000, bytes_accessed=38_000_000, transcendentals=0),
    )(*operands)


def solution(mesh):
    in_specs = []
    for col_split in COLUMN_SPLIT:
        in_specs.extend([grad_spec(col_split), state_spec(col_split), state_spec(col_split), state_spec(col_split)])
    out_specs = tuple([replica_spec(col_split) for col_split in COLUMN_SPLIT] + [state_spec(col_split) for col_split in COLUMN_SPLIT] * 3)
    across, beside = ([(i, partners(i)[k]) for i in PARTNERS] for k in (FAR, NEAR))
    leavers = [(i, k) for i, k in across if i % PAIR == 0]

    def device_step(*arrays):
        shape = jax.ShapeDtypeStruct
        shard = [(LAYERS, rows, cols) for rows, cols in zip(SHARD_ROWS, SHARD_COLS)]
        order = [(kind, piece) for kind in (FCIN, FCOUT) for piece in PIECES[kind - FCIN]]
        scal_shape = (len(KINDS) + 1,) + TILE
        unit = (UNIT_ROWS, UNIT_COLS)
        out_shape = (
            [shape(s, F32) for s in shard]
            + [shape((LAYERS, len(PARTNERS) * SHARD_ROWS[kind], SHARD_COLS[kind]), BF16) for kind in (PROJ, QKV)]
            + [shape((1, rows, SHARD_COLS[kind]), BF16) for kind, (_, _, rows) in order]
            + [shape((PAIR * count,) + unit, BF16) for count in (LATE_GROUPS, TAIL_GROUPS, TAIL_GROUPS)] + [shape(scal_shape, F32)])
        any_spec = pl.BlockSpec(memory_space=pl.ANY)
        dma = pltpu.SemaphoreType.DMA
        messages = len(KINDS) + PAIR
        operands = [arrays[len(KINDS) * kind + part] for part in PARTNERS for kind in KIND_ORDER]
        results = pl.pallas_call(
            step_kernel,
            out_shape=out_shape,
            in_specs=[any_spec] * len(operands),
            out_specs=[any_spec] * len(out_shape),
            scratch_shapes=[
                pltpu.VMEM((len(OTHERS), UNITS) + unit, BF16),
                pltpu.VMEM((PAIR,) + unit, F32),
                pltpu.VMEM((len(OTHERS) * PAIR * SEND_SLOTS,) + unit, BF16),
                pltpu.VMEM((UNITS,) + unit, F32),
                pltpu.VMEM((UNITS,) + unit, F32),
                pltpu.VMEM((RING, len(PARTNERS)) + unit, F32),
                pltpu.VMEM((messages,) + TILE, F32),
                pltpu.VMEM((messages, mesh.size - 1) + TILE, F32),
                pltpu.VMEM((LAYERS * len(KINDS),) + TILE, F32),
                pltpu.VMEM((LAYERS * len(KINDS),) + TILE, F32),
                pltpu.VMEM(TILE, F32),
                pltpu.VMEM(scal_shape, F32),
                dma((RING,)), dma((RING,)), dma((SEND_SLOTS,)), dma((SEND_SLOTS,)), dma((GROUPS,)), dma((len(OTHERS),)), dma((PAIR, messages + PAIR)),
            ],
            compiler_params=pltpu.CompilerParams(collective_id=0, has_side_effects=True, vmem_limit_bytes=66_900_000),
        )(*operands)
        means, reps, pieces, (late, tail, extra, scal) = split(results, len(KINDS), PAIR, PIECE_COUNT, 4)
        data = lax.axis_index("data")
        owners = partners(data)
        state = {}
        clip = scal[len(KINDS), 0, 0]
        for slot, kind in enumerate(KIND_ORDER):
            _, weight, moment1, moment2 = arrays[len(KINDS) * kind:len(KINDS) * kind + len(KINDS)]
            update, new_first, new_second = adam_direction(means[slot], weight, moment1, moment2, clip)
            ratio = jnp.expand_dims(scal[slot, :LAYERS, 0], (1, 2))
            state[kind] = (weight - LEARN_RATE * ratio * update, new_first, new_second)
        far, near = [], []
        for piece in pieces:
            far.append(lax.ppermute(piece, "data", across))
        arrived = lax.ppermute(extra, "data", leavers)
        far_parts = (late, jnp.where(data % PAIR == 0, arrived, tail))
        cross_parts = [lax.ppermute(part, "data", beside) for part in far_parts]
        near = [lax.ppermute(piece, "data", beside) for piece in pieces]
        replicas = list(assemble(reps, far_parts, cross_parts, pieces, near))
        for number, (kind, (layer, first, _)) in enumerate(order):
            far_near = lax.ppermute(far[number], "data", beside)
            for piece, k in ((far[number], FAR), (far_near, CROSS)):
                replicas[kind] = lax.dynamic_update_slice(replicas[kind], piece, (layer, owners[k] * SHARD_ROWS[kind] + first, 0))
        outputs = [replicas[KIND_ORDER.index(kind)] for kind in KINDS]
        return tuple(outputs + [state[kind][part] for part in range(len(OTHERS)) for kind in KINDS])

    return jax.shard_map(device_step, mesh=mesh, in_specs=tuple(in_specs), out_specs=out_specs, check_vma=False)
```

```python
import functools

import jax
import jax.numpy as jnp
from jax import lax
from jax.experimental import pallas as pl
from jax.experimental.pallas import tpu as pltpu
from jax.sharding import PartitionSpec as P


LEARN_RATE = 0.08
BETA_ONE = 0.9
BETA_TWO = 0.999
ADAM_EPS = 1e-6
DECAY_RATE = 0.01
MAX_NORM = 1.0
STEP_COUNT = 100
COLUMN_SPLIT = (True, False, True, False)
MESH = pl.DeviceIdType.MESH
F32, BF16 = jnp.float32, jnp.bfloat16

UNIT_ROWS, UNIT_COLS = 96, 384
CHUNK = 16
PAIR = 2
TILE = (8, 128)
OWN, NEAR, FAR, CROSS = PARTNERS = range(4)
OTHERS = (NEAR, FAR, CROSS)
PROJ, QKV, FCIN, FCOUT = KINDS = range(4)
KIND_ORDER = (1, 0, 2, 3)
SHARD_ROWS = (96, 192, 192, 384)
SHARD_COLS = (768, 1152, 1536, 768)
LAYERS = 4
COL_BLOCKS = tuple(cols // UNIT_COLS for cols in SHARD_COLS)
BLOCKS = tuple(rows // UNIT_ROWS * (cols // UNIT_COLS) for rows, cols in zip(SHARD_ROWS, SHARD_COLS))
FIRST = tuple(sum(LAYERS * blocks for blocks in BLOCKS[:k]) for k in range(5))
UNITS = FIRST[-1]
GROUPS = UNITS // PAIR
RING = 16
SEND_SLOTS = 8
LAG = 8
RESIDENT = PAIR * RING
SENT_UNITS = FIRST[FCIN]
SENT_GROUPS = SENT_UNITS // PAIR
PIECE_UNITS = FIRST[FCOUT] - FIRST[FCIN]
LATE_GROUPS = 2
TAIL_GROUPS = 5
TAIL_FIRST = SENT_GROUPS - TAIL_GROUPS
RELAYED = TAIL_FIRST - LATE_GROUPS
AHEAD = 1
LAST_ROWS = 192
PIECES = tuple(
    [(layer, 0, SHARD_ROWS[kind]) for layer in range(LAYERS - (kind == FCOUT))]
    + [(LAYERS - 1, 0, SHARD_ROWS[kind] - LAST_ROWS), (LAYERS - 1, SHARD_ROWS[kind] - LAST_ROWS, LAST_ROWS)] * (kind == FCOUT)
    for kind in (FCIN, FCOUT))
PIECE_COUNT = sum(map(len, PIECES))


def grad_spec(col_split):
    return P("data", None, None, "model") if col_split else P("data", None, "model", None)


def state_spec(col_split):
    return P(None, "data", "model") if col_split else P(None, ("model", "data"), None)


def replica_spec(col_split):
    return P(None, None, "model") if col_split else P(None, "model", None)


def adam_direction(grad_mean, weight, moment1, moment2, clip_coef):
    clipped = clip_coef * grad_mean
    new_first = BETA_ONE * moment1 + (1.0 - BETA_ONE) * clipped
    new_second = BETA_TWO * moment2 + (1.0 - BETA_TWO) * clipped * clipped
    first_hat = new_first / (1.0 - BETA_ONE ** STEP_COUNT)
    second_hat = new_second / (1.0 - BETA_TWO ** STEP_COUNT)
    update = first_hat / (jnp.sqrt(second_hat) + ADAM_EPS) + DECAY_RATE * weight
    return update, new_first, new_second


def fold(x):
    sublanes, lanes = TILE
    parts = [x[i:i + sublanes, j:j + lanes] for i in range(0, CHUNK, sublanes) for j in range(0, UNIT_COLS, lanes)]
    return functools.reduce(jnp.add, parts)


def pair(group):
    return pl.ds(PAIR * group, PAIR)


def partners(data):
    return data, data + 1 - PAIR * (data % PAIR), (data + PAIR) % len(PARTNERS), CROSS - data


def zeros():
    return jnp.zeros(TILE, F32)


def split(items, *counts):
    items = iter(items)
    return [[next(items) for _ in range(count)] for count in counts]


def place(kind, index):
    blocks, col_blocks = BLOCKS[kind], COL_BLOCKS[kind]
    layer, block = index // blocks, index % blocks
    row = pl.multiple_of(block // col_blocks * UNIT_ROWS, UNIT_ROWS)
    col = pl.multiple_of(block % col_blocks * UNIT_COLS, UNIT_COLS)
    return layer, row, col


def for_kind(unit, kinds, body):
    for kind in kinds:
        @pl.when((unit >= FIRST[kind]) & (unit < FIRST[kind + 1]))
        def _():
            body(kind, unit - FIRST[kind])


def step_kernel(*refs):
    counts = tuple(map(len, PIECES))
    grads, weights, firsts, seconds, means, reps, in_pieces, out_pieces, rest = split(refs, *[len(KINDS)] * 5, PAIR, *counts, 23)
    pieces = {FCIN: in_pieces, FCOUT: out_pieces}
    (late, tail, extra, scal_out, recv, ahead, stage, mean, held, ring, note, notes, w_sums, u_sums, n_sum, scal,
     ring_sem, held_sem, mean_sem, send_sem, recv_sem, rep_send_sem, note_sem) = rest
    model, data = lax.axis_index("model"), lax.axis_index("data")
    partner = partners(data)
    stays = data % PAIR == 1

    def unit_at(ref, kind, index, quarter_base=None):
        layer, row, col = place(kind, index)
        if quarter_base is not None:
            row = pl.multiple_of(quarter_base * SHARD_ROWS[kind] + row, UNIT_ROWS)
            return ref.at[layer, pl.ds(row, UNIT_ROWS), pl.ds(col, UNIT_COLS)]
        return ref.at[layer, pl.ds(row, UNIT_ROWS), pl.ds(col, UNIT_COLS)]

    def start_grads(unit):
        def body(kind, index):
            for k in PARTNERS:
                pltpu.make_async_copy(unit_at(grads[kind].at[0], kind, index, partner[k]), ring.at[unit % RING, k], ring_sem.at[unit % RING]).start()

        for_kind(unit, KINDS, body)

    def start_moments(unit, kinds):
        slot, part = unit // PAIR % RING, PAIR * (unit % PAIR)

        def body(kind, index):
            pltpu.make_async_copy(unit_at(firsts[kind], kind, index), ring.at[slot, part], ring_sem.at[slot]).start()
            pltpu.make_async_copy(unit_at(seconds[kind], kind, index), ring.at[slot, part + 1], ring_sem.at[slot]).start()

        for_kind(unit, kinds, body)

    def start_weight(unit):
        def body(kind, index):
            pltpu.make_async_copy(unit_at(weights[kind], kind, index), held.at[unit], held_sem.at[unit // PAIR % RING]).start()

        for_kind(unit, KINDS, body)

    def start_mean_out(unit):
        def body(kind, index):
            pltpu.make_async_copy(mean.at[unit], unit_at(means[kind], kind, index), mean_sem.at[unit // PAIR % SEND_SLOTS]).start()

        for_kind(unit, KINDS, body)

    def block(ref, count):
        return ref.at[pl.ds(0, count), pl.ds(0, UNIT_ROWS), pl.ds(0, UNIT_COLS)]

    def wait_ring(slot):
        pltpu.make_async_copy(block(grads[QKV].at[0], len(PARTNERS)), ring.at[slot], ring_sem.at[slot]).wait()

    def wait_weights(group):
        pltpu.make_async_copy(block(weights[QKV], PAIR), held.at[pair(group)], held_sem.at[group % RING]).wait()

    def wait_mean_out(group):
        pltpu.make_async_copy(mean.at[pair(group)], block(means[QKV], PAIR), mean_sem.at[group % SEND_SLOTS]).wait()

    def landed(count):
        return recv.at[0, pl.ds(0, count)]

    def remote(source, target, sent, received, k):
        return pltpu.make_async_remote_copy(source, target, sent, received, device_id=(model, partner[k]), device_id_type=MESH)

    def stage_slot(group, k):
        return group % SEND_SLOTS * len(OTHERS) + k - 1

    def grad_copy(group, k):
        return remote(stage.at[pair(stage_slot(group, k))], recv.at[k - 1, pair(group)], send_sem.at[group % SEND_SLOTS], recv_sem.at[group], k)

    def grad_copies(group):
        count = len(OTHERS) * PAIR
        return remote(landed(count), landed(count), send_sem.at[group % SEND_SLOTS], recv_sem.at[group], FAR)

    early = PAIR
    for unit in range(early):
        start_grads_static(unit, grads, ring, ring_sem, partner)

    barrier = pltpu.get_barrier_semaphore()
    peers = [(side, k) for k in (FAR, CROSS, OWN, NEAR) for side in (1, 0) if side or k]

    def device(peer):
        return (model + peer[0]) % PAIR, partner[peer[1]]

    for peer in peers:
        pl.semaphore_signal(barrier, inc=1, device_id=device(peer), device_id_type=MESH)
    for unit in range(early, RING):
        start_grads_static(unit, grads, ring, ring_sem, partner)

    n_sum[...] = jnp.zeros_like(n_sum)
    note[...] = jnp.zeros_like(note)
    w_sums[...] = jnp.zeros_like(w_sums)
    u_sums[...] = jnp.zeros_like(u_sums)

    def convert(group):
        for j in range(PAIR):
            unit = PAIR * group + j
            wait_ring(unit % RING)

            def rows(i, _):
                at = pl.ds(pl.multiple_of(i * CHUNK, CHUNK), CHUNK)
                for k in OTHERS:
                    stage[PAIR * stage_slot(group, k) + j, at, :] = ring[unit % RING, k, at, :].astype(BF16)
                return 0

            lax.fori_loop(0, UNIT_ROWS // CHUNK, rows, 0)

    def keep_own(group):
        for j in range(PAIR):
            unit = PAIR * group + j

            def rows(i, _):
                at = pl.ds(pl.multiple_of(i * CHUNK, CHUNK), CHUNK)
                mean[unit, at, :] = ring[unit % RING, OWN, at, :].astype(BF16).astype(F32)
                return 0

            lax.fori_loop(0, UNIT_ROWS // CHUNK, rows, 0)

    def add_up(group):
        grad_copies(group).wait_recv()
        wait_weights(group)

        @pl.when(group >= SEND_SLOTS)
        def _():
            wait_mean_out(group - SEND_SLOTS)

        for j in range(PAIR):
            unit = PAIR * group + j

            def rows(i, sums):
                at = pl.ds(pl.multiple_of(i * CHUNK, CHUNK), CHUNK)
                near, far, cross = (recv[k - 1, unit, at, :].astype(F32) for k in OTHERS)
                total = (mean[unit, at, :] + near + (far + cross)) / len(PARTNERS)
                mean[unit, at, :] = total
                weight = held[unit, at, :]
                g_sum, w_sum = sums
                return g_sum + fold(total * total), w_sum + fold(weight * weight)

            g_part, w_part = lax.fori_loop(0, UNIT_ROWS // CHUNK, rows, (zeros(), zeros()))
            n_sum[...] += g_part

            def body(kind, index):
                tensor = LAYERS * kind + index // BLOCKS[kind]
                w_sums[tensor] += w_part

            for_kind(unit, KINDS, body)
            start_mean_out(unit)

    convert(0)
    keep_own(0)
    pl.semaphore_wait(barrier, len(peers))

    def exchange_step(group, _):
        for j in range(PAIR):
            start_weight(PAIR * group + j)

        @pl.when(group >= SEND_SLOTS)
        def _():
            grad_copies(group - SEND_SLOTS).wait_send()

        @pl.when(group >= 1)
        def _():
            convert(group)
            keep_own(group)

        for k in (FAR, CROSS, NEAR):
            grad_copy(group, k).start()

        for j in range(PAIR):
            unit = PAIR * group + j

            @pl.when(unit + RING < UNITS)
            def _():
                start_grads(unit + RING)

            @pl.when(unit + RING >= UNITS)
            def _():
                for other in range(PAIR):
                    start_moments(PAIR * (unit + RING - UNITS) + other, (PROJ, QKV))

        @pl.when(group >= LAG + 1)
        def _():
            add_up(group - LAG - 1)

        return 0

    lax.fori_loop(0, GROUPS, exchange_step, 0)

    def drain_step(group, _):
        add_up(group)
        return 0

    lax.fori_loop(GROUPS - LAG - 1, GROUPS, drain_step, 0)

    n_note, early_note = len(KINDS), len(KINDS) + 1

    def rows_of(index):
        return pl.ds(0, PAIR if index == early_note else 1)

    def send_note(index):
        for slot, peer in enumerate(peers):
            pltpu.make_async_remote_copy(
                note.at[index, rows_of(index)], notes.at[index, slot, rows_of(index)], note_sem.at[0, index], note_sem.at[1, index],
                device_id=device(peer), device_id_type=MESH).start()

    def read_note(index):
        arrived = notes.at[index, pl.ds(0, len(peers)), rows_of(index)]
        remote(arrived, arrived, note_sem.at[0, index], note_sem.at[1, index], FAR).wait()
        return note[index] + jnp.sum(notes[index], axis=0)

    def ahead_copy(part, first_row=0, end_row=UNIT_ROWS):
        rows, sem = pl.ds(first_row, end_row - first_row), len(KINDS) + PAIR + part
        return remote((held, mean)[part].at[AHEAD, rows], ahead.at[part, rows], note_sem.at[0, sem], note_sem.at[1, sem], FAR)

    note[n_note, :1, :] = jnp.sum(n_sum[...], axis=0, keepdims=True)

    def settle(group, _):
        grad_copies(group).wait_send()
        return 0

    lax.fori_loop(GROUPS - SEND_SLOTS, GROUPS, settle, 0)
    send_note(n_note)
    ahead_copy(0).start()

    def settle_means(group, _):
        wait_mean_out(group)
        return 0

    lax.fori_loop(GROUPS - SEND_SLOTS, GROUPS, settle_means, 0)
    total_sq = jnp.sum(read_note(n_note)[:1, :], axis=1, keepdims=True)
    clip = jnp.minimum(1.0, MAX_NORM / jnp.sqrt(total_sq))
    scal[len(KINDS)] = jnp.broadcast_to(clip, TILE)

    def directions(kind, unit_from, unit_to):
        def group_step(index, _):
            group = FIRST[kind] // PAIR + index
            slot = group % RING
            wait_ring(slot)
            total = zeros()
            for j in range(PAIR):
                unit, part = PAIR * group + j, PAIR * j
                for i in range(0, UNIT_ROWS, CHUNK):
                    at = pl.ds(i, CHUNK)
                    update, _, _ = adam_direction(mean[unit, at, :], held[unit, at, :], ring[slot, part, at, :], ring[slot, part + 1, at, :], clip)
                    mean[unit, at, :] = update
                    total = total + fold(update * update)
            u_sums[LAYERS * kind + PAIR * index // BLOCKS[kind]] += total
            return 0

        lax.fori_loop(unit_from // PAIR, unit_to // PAIR, group_step, 0)

    def refill(unit_from, unit_to):
        def unit_step(unit, _):
            start_moments(unit + RESIDENT, (FCIN, FCOUT))
            return 0

        lax.fori_loop(unit_from, unit_to, unit_step, 0)

    def tensor_sums(kind, layers):
        return [jnp.sum(sums[LAYERS * kind + layer], axis=0, keepdims=True) for sums in (u_sums, w_sums) for layer in range(layers)]

    def write_early_note():
        for row, total in enumerate(tensor_sums(PROJ, 1)):
            note[early_note, row:row + 1, :] = total

    def write_note(kind):
        lane = lax.broadcasted_iota(jnp.int32, (1, TILE[1]), 1)
        packed = jnp.zeros((1, TILE[1]), F32)
        for index, total in enumerate(tensor_sums(kind, LAYERS)):
            packed = jnp.where(lane == index, jnp.sum(total, axis=1, keepdims=True), packed)
        note[kind, :1, :] = packed

    def early_ratio():
        norms = jnp.sqrt(jnp.sum(read_note(early_note)[:PAIR, :], axis=1, keepdims=True))
        scal[PROJ, :1, :] = jnp.broadcast_to(norms[1:PAIR] / norms[:1], (1, TILE[1]))

    def ratios(kind):
        norms = jnp.sqrt(read_note(kind)[:1, :])
        for layer in range(LAYERS):
            ratio = norms[:, LAYERS + layer:LAYERS + layer + 1] / norms[:, layer:layer + 1]
            scal[kind, layer:layer + 1, :] = jnp.broadcast_to(ratio, (1, TILE[1]))

    def new_weights(kind, unit_from, unit_to, target):
        def unit_step(index, _):
            unit = FIRST[kind] + index
            ratio = LEARN_RATE * scal[kind, pl.ds(index // BLOCKS[kind], 1), :][:, :1]
            for i in range(0, UNIT_ROWS, CHUNK):
                at = pl.ds(i, CHUNK)
                target[unit, at, :] = (held[unit, at, :] - ratio * mean[unit, at, :]).astype(BF16)
            return 0

        lax.fori_loop(unit_from, unit_to, unit_step, 0)

    def weights_ahead():
        ratio = LEARN_RATE * scal[PROJ, AHEAD // BLOCKS[PROJ]:AHEAD // BLOCKS[PROJ] + 1, :][:, :1]
        for i in range(0, UNIT_ROWS, CHUNK):
            at = pl.ds(i, CHUNK)
            recv[FAR - 1, AHEAD, at, :] = (ahead[0, at, :] - ratio * ahead[1, at, :]).astype(BF16)

    near_sem = PAIR * SENT_GROUPS

    def rep_copy(group, k):
        source = recv.at[FAR - 1, pair(group)] if k == CROSS else stage.at[pair(group)]
        arrival = {NEAR: near_sem, FAR: group, CROSS: SENT_GROUPS + group}[k]
        return remote(source, recv.at[k - 1, pair(group)], rep_send_sem.at[k - 1], recv_sem.at[arrival], FAR if k == FAR else NEAR)

    def first_copy():
        return remote(stage.at[0], recv.at[FAR - 1, 0], rep_send_sem.at[FAR - 1], recv_sem.at[0], FAR)

    def late_copy(group):
        target = late.at[pair(group - RELAYED)] if group < TAIL_FIRST else tail.at[pair(group - TAIL_FIRST)]
        return remote(stage.at[pair(group)], target, rep_send_sem.at[FAR - 1], recv_sem.at[group], FAR)

    def all_copies(k, count):
        return remote(landed(count), landed(count), rep_send_sem.at[k - 1], recv_sem.at[near_sem], NEAR)

    def start_replicas(unit_from, unit_to):
        def body(group, _):
            rep_copy(group, FAR).start()
            rep_copy(group, NEAR).start()
            return 0

        lax.fori_loop(unit_from // PAIR, unit_to // PAIR, body, 0)

    def start_late_replicas():
        for group in range(RELAYED, SENT_GROUPS):
            if group < TAIL_FIRST:
                late_copy(group).start()
            else:
                pl.when(stays)(late_copy(group).start)
            rep_copy(group, NEAR).start()

    def replicas_out(unit_from, unit_to, k):
        def unit_step(unit, _):
            def body(kind, index):
                source = recv.at[k - 1, unit] if k else stage.at[unit]
                pltpu.make_async_copy(source, unit_at(reps[kind], kind, index, partner[k]), mean_sem.at[k]).start()

            for_kind(unit, (PROJ, QKV), body)
            return 0

        lax.fori_loop(unit_from, unit_to, unit_step, 0)

    def pieces_out(kind):
        for ref, (layer, first, rows) in zip(pieces[kind], PIECES[kind - FCIN]):
            for row in range(0, rows, UNIT_ROWS):
                for column in range(COL_BLOCKS[kind]):
                    unit = FIRST[kind] + layer * BLOCKS[kind] + (first + row) // UNIT_ROWS * COL_BLOCKS[kind] + column
                    target = ref.at[0, pl.ds(row, UNIT_ROWS), pl.ds(column * UNIT_COLS, UNIT_COLS)]
                    pltpu.make_async_copy(recv.at[0, unit], target, mean_sem.at[PAIR + kind]).start()

    proj_end, qkv_end, piece_end = (FIRST[kind + 1] - FIRST[kind] for kind in (PROJ, QKV, FCIN))
    first, half = BLOCKS[PROJ], qkv_end // PAIR
    directions(PROJ, 0, first)
    write_early_note()
    refill(0, first)
    send_note(early_note)
    ahead_copy(1, 0, CHUNK * PAIR).start()
    directions(PROJ, first, proj_end)
    write_note(PROJ)
    refill(first, PAIR * first)
    send_note(PROJ)
    ahead_copy(1, CHUNK * PAIR).start()
    directions(QKV, 0, half)
    early_ratio()
    new_weights(PROJ, 0, first, stage)
    refill(PAIR * first, PAIR * first + PAIR)
    first_copy().start()
    rep_copy(0, NEAR).start()
    ratios(PROJ)
    new_weights(PROJ, first, proj_end, stage)
    refill(PAIR * first + PAIR, proj_end)
    start_replicas(first, PAIR * first)
    directions(QKV, half, qkv_end)
    write_note(QKV)
    refill(proj_end, proj_end + PAIR)
    send_note(QKV)
    refill(proj_end + PAIR, SENT_UNITS)
    start_replicas(PAIR * first, proj_end)
    directions(FCIN, 0, piece_end // PAIR)
    ratios(QKV)
    new_weights(QKV, 0, half, stage)
    directions(FCIN, piece_end // PAIR, piece_end // PAIR + PAIR)
    start_replicas(proj_end, proj_end + half // PAIR)
    directions(FCIN, piece_end // PAIR + PAIR, piece_end)
    refill(FIRST[FCIN], FIRST[FCOUT])
    new_weights(QKV, half, qkv_end, stage)
    directions(FCOUT, 0, piece_end)
    write_note(FCIN)
    write_note(FCOUT)
    extra_copy = pltpu.make_async_copy(stage.at[pl.ds(PAIR * TAIL_FIRST, PAIR * TAIL_GROUPS)], extra, mean_sem.at[SEND_SLOTS - 1])
    extra_copy.start()
    send_note(FCIN)
    send_note(FCOUT)
    start_replicas(proj_end + half // PAIR, PAIR * RELAYED)
    start_late_replicas()
    for part in range(PAIR):
        ahead_copy(part).wait()
    weights_ahead()
    replicas_out(0, SENT_UNITS, OWN)
    for kind in (FCIN, FCOUT):
        ratios(kind)
        new_weights(kind, 0, piece_end, recv.at[0])
    scal_copy = pltpu.make_async_copy(scal, scal_out, mean_sem.at[len(KINDS) + PAIR])
    scal_copy.start()
    pieces_out(FCIN)
    pieces_out(FCOUT)
    all_copies(NEAR, SENT_UNITS).wait()
    replicas_out(0, SENT_UNITS, NEAR)

    def relay_step(group, _):
        @pl.when(group < RELAYED)
        def _():
            @pl.when(group == 0)
            def _():
                first_copy().wait_recv()

            @pl.when(group >= 1)
            def _():
                rep_copy(group, FAR).wait_recv()

            rep_copy(group, CROSS).start()
            replicas_out(PAIR * group, PAIR * group + PAIR, FAR)

        @pl.when(group >= 1)
        def _():
            rep_copy(group - 1, CROSS).wait_recv()
            replicas_out(PAIR * group - PAIR, PAIR * group, CROSS)

        return 0

    lax.fori_loop(0, RELAYED + 1, relay_step, 0)
    all_copies(CROSS, PAIR * RELAYED).wait_send()
    for index, count in enumerate((SENT_UNITS, SENT_UNITS, PAIR * RELAYED, PAIR * RELAYED, PIECE_UNITS, PIECE_UNITS)):
        pltpu.make_async_copy(landed(count), landed(count), mean_sem.at[index]).wait()
    scal_copy.wait()
    extra_copy.wait()
    for group in range(RELAYED, TAIL_FIRST):
        late_copy(group).wait_recv()

    @pl.when(stays)
    def _():
        all_copies(FAR, SENT_UNITS - 1).wait_send()
        for group in range(TAIL_FIRST, SENT_GROUPS):
            late_copy(group).wait_recv()

    @pl.when(jnp.logical_not(stays))
    def _():
        all_copies(FAR, PAIR * TAIL_FIRST - 1).wait_send()


def place_static(kind, index):
    block = index % BLOCKS[kind]
    return index // BLOCKS[kind], block // COL_BLOCKS[kind] * UNIT_ROWS, block % COL_BLOCKS[kind] * UNIT_COLS


def start_grads_static(unit, grads, ring, ring_sem, partner):
    kind = next(kind for kind in KINDS if unit < FIRST[kind + 1])
    layer, row, col = place_static(kind, unit - FIRST[kind])
    for k in (FAR, CROSS, NEAR, OWN):
        base = pl.multiple_of(partner[k] * SHARD_ROWS[kind] + row, UNIT_ROWS)
        pltpu.make_async_copy(grads[kind].at[0, layer, pl.ds(base, UNIT_ROWS), pl.ds(col, UNIT_COLS)], ring.at[unit, k], ring_sem.at[unit]).start()


def assemble_kernel(*refs):
    (proj, qkv), far_parts, cross_parts, own, near, outs, scratch = split(refs, PAIR, PAIR, PAIR, PIECE_COUNT, PIECE_COUNT, len(KINDS), 7)
    proj_buf, qkv_buf, in_buf, out_buf, late_sem, whole_sem, piece_sem = scratch
    partner = partners(lax.axis_index("data"))
    copies = []

    def through(source, buffer, target, sem):
        copies.append((pltpu.make_async_copy(source, buffer, sem.at[0]), pltpu.make_async_copy(buffer, target, sem.at[1])))

    for layer in range(LAYERS):
        through(qkv.at[layer], qkv_buf.at[layer], outs[QKV].at[layer], whole_sem.at[layer])
    through(proj, proj_buf, outs[PROJ], whole_sem.at[LAYERS])
    order = [(kind, piece) for kind in (FCIN, FCOUT) for piece in PIECES[kind - FCIN]]
    for number, (kind, (layer, first, rows)) in enumerate(order):
        for k, piece in ((OWN, own[number]), (NEAR, near[number])):
            at = (in_buf if kind == FCIN else out_buf).at[k, pl.ds(layer, 1), pl.ds(first, rows)]
            base = pl.multiple_of(partner[k] * SHARD_ROWS[kind] + first, UNIT_ROWS)
            through(piece, at, outs[kind].at[pl.ds(layer, 1), pl.ds(base, rows)], piece_sem.at[k, number])
    fills = [[] for _ in range(LAYERS)]
    for k, sources in ((FAR, far_parts), (CROSS, cross_parts)):
        units = [source.at[unit] for source in sources for unit in range(source.shape[0])]
        for number, source in enumerate(units):
            layer, row, col = place_static(QKV, PAIR * RELAYED + number - FIRST[QKV])
            base = pl.multiple_of(partner[k] * SHARD_ROWS[QKV] + row, UNIT_ROWS)
            target = qkv_buf.at[layer, pl.ds(base, UNIT_ROWS), pl.ds(col, UNIT_COLS)]
            fills[layer].append(pltpu.make_async_copy(source, target, late_sem.at[k - FAR, number]))
    for fetch, _ in copies:
        fetch.start()
    for (fetch, _), layer_fills in zip(copies, fills):
        fetch.wait()
        for fill in layer_fills:
            fill.start()
    for (_, store), layer_fills in zip(copies, fills):
        for fill in layer_fills:
            fill.wait()
        store.start()
    for fetch, store in copies[LAYERS:]:
        fetch.wait()
        store.start()
    for _, store in copies:
        store.wait()


def assemble(reps, far_parts, cross_parts, own, near):
    shape, dma = jax.ShapeDtypeStruct, pltpu.SemaphoreType.DMA
    whole = [(LAYERS, len(PARTNERS) * rows, cols) for rows, cols in zip(SHARD_ROWS, SHARD_COLS)]
    any_spec = pl.BlockSpec(memory_space=pl.ANY)
    operands = [*reps, *far_parts, *cross_parts, *own, *near]
    return pl.pallas_call(
        assemble_kernel,
        out_shape=[shape(s, BF16) for s in whole],
        in_specs=[any_spec] * len(operands),
        out_specs=[any_spec] * len(whole),
        scratch_shapes=[
            pltpu.VMEM(whole[PROJ], BF16),
            pltpu.VMEM(whole[QKV], BF16),
            pltpu.VMEM((PAIR, LAYERS, SHARD_ROWS[FCIN], SHARD_COLS[FCIN]), BF16),
            pltpu.VMEM((PAIR, LAYERS, SHARD_ROWS[FCOUT], SHARD_COLS[FCOUT]), BF16),
            dma((PAIR, SENT_UNITS - PAIR * RELAYED)), dma((LAYERS + 1, PAIR)), dma((PAIR, len(own), PAIR)),
        ],
        compiler_params=pltpu.CompilerParams(vmem_limit_bytes=24_000_000),
        cost_estimate=pl.CostEstimate(flops=12_000_000, bytes_accessed=38_000_000, transcendentals=0),
    )(*operands)


def solution(mesh):
    in_specs = []
    for col_split in COLUMN_SPLIT:
        in_specs.extend([grad_spec(col_split), state_spec(col_split), state_spec(col_split), state_spec(col_split)])
    out_specs = tuple([replica_spec(col_split) for col_split in COLUMN_SPLIT] + [state_spec(col_split) for col_split in COLUMN_SPLIT] * 3)
    across, beside = ([(i, partners(i)[k]) for i in PARTNERS] for k in (FAR, NEAR))
    leavers = [(i, k) for i, k in across if i % PAIR == 0]

    def device_step(*arrays):
        shape = jax.ShapeDtypeStruct
        shard = [(LAYERS, rows, cols) for rows, cols in zip(SHARD_ROWS, SHARD_COLS)]
        order = [(kind, piece) for kind in (FCIN, FCOUT) for piece in PIECES[kind - FCIN]]
        scal_shape = (len(KINDS) + 1,) + TILE
        unit = (UNIT_ROWS, UNIT_COLS)
        out_shape = (
            [shape(s, F32) for s in shard]
            + [shape((LAYERS, len(PARTNERS) * SHARD_ROWS[kind], SHARD_COLS[kind]), BF16) for kind in (PROJ, QKV)]
            + [shape((1, rows, SHARD_COLS[kind]), BF16) for kind, (_, _, rows) in order]
            + [shape((PAIR * count,) + unit, BF16) for count in (LATE_GROUPS, TAIL_GROUPS, TAIL_GROUPS)] + [shape(scal_shape, F32)])
        any_spec = pl.BlockSpec(memory_space=pl.ANY)
        dma = pltpu.SemaphoreType.DMA
        messages = len(KINDS) + PAIR
        operands = [arrays[len(KINDS) * kind + part] for part in PARTNERS for kind in KIND_ORDER]
        results = pl.pallas_call(
            step_kernel,
            out_shape=out_shape,
            in_specs=[any_spec] * len(operands),
            out_specs=[any_spec] * len(out_shape),
            scratch_shapes=[
                pltpu.VMEM((len(OTHERS), UNITS) + unit, BF16),
                pltpu.VMEM((PAIR,) + unit, F32),
                pltpu.VMEM((len(OTHERS) * PAIR * SEND_SLOTS,) + unit, BF16),
                pltpu.VMEM((UNITS,) + unit, F32),
                pltpu.VMEM((UNITS,) + unit, F32),
                pltpu.VMEM((RING, len(PARTNERS)) + unit, F32),
                pltpu.VMEM((messages,) + TILE, F32),
                pltpu.VMEM((messages, mesh.size - 1) + TILE, F32),
                pltpu.VMEM((LAYERS * len(KINDS),) + TILE, F32),
                pltpu.VMEM((LAYERS * len(KINDS),) + TILE, F32),
                pltpu.VMEM(TILE, F32),
                pltpu.VMEM(scal_shape, F32),
                dma((RING,)), dma((RING,)), dma((SEND_SLOTS,)), dma((SEND_SLOTS,)), dma((GROUPS,)), dma((len(OTHERS),)), dma((PAIR, messages + PAIR)),
            ],
            compiler_params=pltpu.CompilerParams(collective_id=0, has_side_effects=True, vmem_limit_bytes=66_900_000),
        )(*operands)
        means, reps, pieces, (late, tail, extra, scal) = split(results, len(KINDS), PAIR, PIECE_COUNT, 4)
        data = lax.axis_index("data")
        owners = partners(data)
        state = {}
        clip = scal[len(KINDS), 0, 0]
        for slot, kind in enumerate(KIND_ORDER):
            _, weight, moment1, moment2 = arrays[len(KINDS) * kind:len(KINDS) * kind + len(KINDS)]
            update, new_first, new_second = adam_direction(means[slot], weight, moment1, moment2, clip)
            ratio = jnp.expand_dims(scal[slot, :LAYERS, 0], (1, 2))
            state[kind] = (weight - LEARN_RATE * ratio * update, new_first, new_second)
        far, near = [], []
        for piece in pieces:
            far.append(lax.ppermute(piece, "data", across))
        arrived = lax.ppermute(extra, "data", leavers)
        far_parts = (late, jnp.where(data % PAIR == 0, arrived, tail))
        cross_parts = [lax.ppermute(part, "data", beside) for part in far_parts]
        near = [lax.ppermute(piece, "data", beside) for piece in pieces]
        replicas = list(assemble(reps, far_parts, cross_parts, pieces, near))
        for number, (kind, (layer, first, _)) in enumerate(order):
            far_near = lax.ppermute(far[number], "data", beside)
            for piece, k in ((far[number], FAR), (far_near, CROSS)):
                replicas[kind] = lax.dynamic_update_slice(replicas[kind], piece, (layer, owners[k] * SHARD_ROWS[kind] + first, 0))
        outputs = [replicas[KIND_ORDER.index(kind)] for kind in KINDS]
        return tuple(outputs + [state[kind][part] for part in range(len(OTHERS)) for kind in KINDS])

    return jax.shard_map(device_step, mesh=mesh, in_specs=tuple(in_specs), out_specs=out_specs, check_vma=False)
```
